128 devices in a mesh: tm: 16 (over y_hi, z, core), dp: 8 (over x, y_lo).
Axes of the slice: x: 4, y: 4 (y_hi: 2, y_lo: 2; y = y_hi * 2 + y_lo), z: 4, core: 2. Of those that a mesh axis runs over, the one named last changes fastest.
Arguments:
- encoded: bfloat16 [2048, 80, 1024], P('dp', 'tm'), may hold values from -6 to 6
- queries: bfloat16 [2048, 32, 1024], P(('dp', 'tm')), may hold values from -200 to 200
- cotangent: bfloat16 [2048, 32, 1024], P(('dp', 'tm')), may hold values from -0.044433594 to 0.044433594
- lengths: int32 [2048], P(('dp', 'tm')), may hold values from 2 to 80
- key_weight: bfloat16 [1024, 1024], replicated, may hold values from -0.1875 to 0.1875
- value_weight: bfloat16 [1024, 1024], replicated, may hold values from -0.1875 to 0.1875
Outputs:
- context: bfloat16 [2048, 32, 1024], P(('dp', 'tm'))
- key_grad: float32 [1024, 1024], replicated
- value_grad: float32 [1024, 1024], replicated
The draws below stay inside these ranges and needn't reach their ends.
Inputs may be any that keep to these rules, and one draw needn't show every extreme that they name: Sequence b attends only to source positions below lengths[b].
All inputs are finite; a program needn't handle non-finite values.
Results may differ from the reference program's by a relative error of at most 0.0069.
Values may be sent and summed in bfloat16 or wider, within the bound.
A program may use at most 128 MiB of HBM per device.

```python
import math
import jax
import jax.numpy as jnp
from jax import lax

D = 1024
SRC = 80
TGT = 32
SEQ_DEV = 16
BATCH = 2048
N_DP = 8


def encoded_values(key):
    base = jax.random.fold_in(key, 11)
    drawn = jax.random.truncated_normal(base, -6.0, 6.0, (BATCH, SRC, D), jnp.float32)
    return drawn.astype(jnp.bfloat16)


def key_matrix(key):
    base = jax.random.fold_in(key, 12)
    drawn = jax.random.truncated_normal(base, -6.0, 6.0, (D, D), jnp.float32) / math.sqrt(D)
    return drawn.astype(jnp.bfloat16)


def draw_encoded(key, part):
    return encoded_values(key)


def draw_key_weight(key, part):
    return key_matrix(key)


def draw_queries(key, part):
    base = jax.random.fold_in(key, 13)
    drawn = jax.random.truncated_normal(base, -6.0, 6.0, (BATCH, TGT, D), jnp.float32)
    return drawn.astype(jnp.bfloat16)


def place_ends(result, rng, least, high):
    shape = result.shape
    spot = [jax.random.randint(jax.random.fold_in(rng, axis), (), 0, shape[axis]) for axis in range(len(shape))]
    result = result.at[tuple(spot)].set(least)
    longest = shape.index(max(shape))
    spot[longest] = (spot[longest] + 1) % shape[longest]
    return result.at[tuple(spot)].set(high)


def level_of(rng, extent, shards, smallest, high):
    def one(position, blocks):
        heights = jax.random.uniform(jax.random.fold_in(jax.random.fold_in(rng, 6), position), (blocks,), jnp.float32, smallest / len(shards), high / len(shards))
        return jnp.repeat(jnp.exp(heights), extent[position] // blocks).reshape((-1,) + (1,) * (len(extent) - position - 1))

    gain = one(*shards[0])
    for cut in shards[1:]:
        gain = gain * one(*cut)
    return gain


def normal_values(stream_key, shape, deviation, bound, split=(), kind=jnp.bfloat16):
    entries = jax.random.normal(stream_key, shape, jnp.float32) * deviation
    if len(split) > 0:
        entries = level_of(stream_key, shape, split, -0.22, 0.18) * entries
    return jnp.clip(entries, min=-bound, max=bound).astype(kind)


def setup_inputs(seed: int = 0) -> dict:
    seeds = jax.random.split(jax.random.key(seed), 7)
    encoded = draw_encoded(jax.random.fold_in(seeds[6], 71), 0)
    queries = draw_queries(jax.random.fold_in(seeds[6], 71), 0)
    cotangent = normal_values(seeds[2], (BATCH, TGT, D), (3.0 / (BATCH * SRC) ** 0.5), 0.044433594, ((0, 128),))
    lengths = place_ends(jax.random.randint(seeds[3], (BATCH,), 2, SRC + 1), jax.random.fold_in(seeds[3], 1), 2, SRC).astype(jnp.int32)
    key_weight = draw_key_weight(jax.random.fold_in(seeds[6], 71), 0)
    value_weight = normal_values(seeds[5], (D, D), D ** -0.5, 0.1875)
    return dict(encoded=encoded, queries=queries, cotangent=cotangent, lengths=lengths, key_weight=key_weight, value_weight=value_weight)


def attend(queries, key_rows, value_rows, lengths, cotangent):
    score_scale = 1.0 / math.sqrt(queries.shape[-1])
    scores = jnp.einsum('btd,bsd->bts', queries.astype(jnp.float32), key_rows.astype(jnp.float32)) * score_scale
    positions = jnp.arange(key_rows.shape[1], dtype=jnp.int32)
    in_range = positions[None, None, :] < lengths[:, None, None]
    scores = jnp.where(in_range, scores, -1e+30)
    row_max = lax.optimization_barrier(jnp.max(scores, axis=-1, keepdims=True))
    weights = jnp.exp(scores - row_max)
    probabilities = weights / lax.optimization_barrier(jnp.sum(weights, axis=-1, keepdims=True))
    probs_low = lax.optimization_barrier(probabilities.astype(jnp.bfloat16))
    context = jnp.einsum('bts,bsd->btd', probs_low.astype(jnp.float32), value_rows.astype(jnp.float32)).astype(jnp.bfloat16)
    grad_probs = jnp.einsum('btd,bsd->bts', cotangent.astype(jnp.float32), value_rows.astype(jnp.float32))
    grad_scores = probabilities * (grad_probs - lax.optimization_barrier(jnp.sum(probabilities * grad_probs, axis=-1, keepdims=True)))
    grad_low = lax.optimization_barrier(grad_scores.astype(jnp.bfloat16))
    grad_values = jnp.einsum('bts,btd->bsd', probs_low.astype(jnp.float32), cotangent.astype(jnp.float32)).astype(jnp.bfloat16)
    grad_keys = (jnp.einsum('bts,btd->bsd', grad_low.astype(jnp.float32), queries.astype(jnp.float32)) * score_scale).astype(jnp.bfloat16)
    return (context, grad_keys, grad_values)

def reference(encoded, queries, cotangent, lengths, key_weight, value_weight):
    block_rows = SEQ_DEV * N_DP
    block_count = BATCH // block_rows
    enc_blocks = encoded.reshape(block_count, block_rows, SRC, D)
    query_blocks = queries.reshape(block_count, block_rows, TGT, D)
    cotan_blocks = cotangent.reshape(block_count, block_rows, TGT, D)
    length_blocks = lengths.reshape(block_count, block_rows)

    def scan_step(totals, pieces):
        enc_block, query_block, cotan_block, length_block = pieces
        flattened = enc_block.reshape(-1, D)
        key_rows = jnp.dot(flattened, key_weight, preferred_element_type=jnp.float32).astype(jnp.bfloat16).reshape(block_rows, SRC, D)
        value_rows = jnp.dot(flattened, value_weight, preferred_element_type=jnp.float32).astype(jnp.bfloat16).reshape(block_rows, SRC, D)
        context, grad_keys, grad_values = attend(query_block, key_rows, value_rows, length_block, cotan_block)
        key_total = totals[0] + jnp.dot(flattened.T, grad_keys.reshape(-1, D), preferred_element_type=jnp.float32)
        value_total = totals[1] + jnp.dot(flattened.T, grad_values.reshape(-1, D), preferred_element_type=jnp.float32)
        return ((key_total, value_total), context)
    zeros = jnp.zeros((D, D), jnp.float32)
    totals, contexts = lax.scan(scan_step, (zeros, zeros), (enc_blocks, query_blocks, cotan_blocks, length_blocks))
    return (contexts.reshape(BATCH, TGT, D), totals[0], totals[1])
```

```python
import functools

import jax
import jax.numpy as jnp
from jax import lax
from jax.experimental import pallas as pl
from jax.experimental.pallas import tpu as pltpu
from jax.sharding import PartitionSpec as P

MESH = pl.DeviceIdType.MESH
F32, BF16 = jnp.float32, jnp.bfloat16
OFFS = (
    (0, 0, 0), (0, 0, 1),
    (0, 1, 0), (0, 3, 0), (1, 0, 0), (0, 1, 1), (0, 3, 1), (1, 0, 1),
    (1, 1, 0), (1, 3, 0), (0, 2, 0), (1, 1, 1), (1, 3, 1), (0, 2, 1),
    (1, 2, 0), (1, 2, 1),
)
GROUPS = ((0, 384, (0, 1, 2)), (384, 768, (1, 2, 0)), (768, 1024, (2, 0, 1)))
HOPS = (2, 1, 3)
SIZES = (256, 64, 16)


def nt(a, b):
    return lax.dot_general(a, b, (((1,), (1,)), ((), ())), preferred_element_type=F32)


def nn(a, b):
    return jnp.dot(a, b, preferred_element_type=F32)


def tn(a, b):
    return lax.dot_general(a, b, (((0,), (0,)), ((), ())), preferred_element_type=F32)


def kernel(
    enc, q, cot, lens, wk, wv, grads, ctx,
    e, et, v, st, gp, pg, qc, w, a, a_in, r_in, own, snd, rcv, rcv2, rcv3, res, ctxb,
    lsem, xs, xr, ds, dr, gs, gr, fs, fr, osem,
):
    tm, dp = lax.axis_index("tm"), lax.axis_index("dp")
    yh, z, c = tm // 8, (tm // 2) % 4, tm % 2
    x, y = dp // 2, yh * 2 + dp % 2
    at = (x, y, z)

    def device(x, y, z, c):
        return ((y // 2) * 8 + z * 2 + c, x * 2 + y % 2)

    def tm_at(off, sign):
        return ((yh + off[0]) % 2) * 8 + ((z + sign * off[1] + 4) % 4) * 2 + (c + off[2]) % 2

    def along(axis, hop):
        there = list(at)
        there[axis] = (there[axis] + hop) % 4
        return device(*there, c)

    partner = device(x, y, z, 1 - c)

    local = [
        pltpu.make_async_copy(q, qc.at[0], lsem.at[0]),
        pltpu.make_async_copy(cot, qc.at[1], lsem.at[1]),
        pltpu.make_async_copy(wk, w.at[0], lsem.at[2]),
        pltpu.make_async_copy(wv, w.at[1], lsem.at[3]),
        pltpu.make_async_copy(
            enc.at[:, pl.ds(pl.multiple_of(16 * tm, 16), 16)], e.at[pl.ds(0, 5)], lsem.at[4]
        ),
    ]
    barrier = pltpu.get_barrier_semaphore()
    peers = [(tm_at(off, 1), dp) for off in OFFS[1:]]
    peers += [along(0, h) for h in (1, 2, 3)] + [along(1, h) for h in (1, 3)]
    for peer in peers:
        pl.semaphore_signal(barrier, inc=1, device_id=peer, device_id_type=MESH)
    for copy in local:
        copy.start()
    pl.semaphore_wait(barrier, len(peers))

    def exchange(k, target):
        return pltpu.make_async_remote_copy(
            src_ref=enc.at[:, pl.ds(pl.multiple_of(16 * target, 16), 16)],
            dst_ref=e.at[pl.ds(5 * k, 5)],
            send_sem=xs.at[k],
            recv_sem=xr.at[k],
            device_id=(target, dp),
            device_id_type=MESH,
        )

    sends = []
    for k, off in enumerate(OFFS):
        if k:
            copy = exchange(k, tm_at(off, 1))
            copy.start()
            sends.append(copy)
    for copy in local[:2]:
        copy.wait()

    def to_partner(src, dst, k):
        return pltpu.make_async_remote_copy(
            src_ref=src, dst_ref=dst, send_sem=ds.at[k], recv_sem=dr.at[k],
            device_id=partner, device_id_type=MESH,
        )

    operand = to_partner(qc.at[1 - c], r_in, 0)
    operand.start()
    sends.append(operand)

    column = lax.broadcasted_iota(jnp.int32, (1, 512), 1) // 32
    limit = jnp.zeros((1, 512), jnp.int32)
    for b in range(16):
        limit = jnp.where(column == b, lens[b], limit)
    row = lax.broadcasted_iota(jnp.int32, (80, 512), 0)
    same = row % 16 == column
    for k, off in enumerate(OFFS):
        position = 5 * tm_at(off, -1) + row // 16
        st[pl.ds(80 * k, 80), :] = jnp.where(same & (position < limit), 0.0, -1e30)

    for copy in local[2:]:
        copy.wait()

    def arrive(j, carry):
        top, total, dots = carry
        for i in range(3):
            k = 3 * j + 1 + i
            pltpu.make_async_remote_copy(
                src_ref=enc.at[:, pl.ds(0, 16)],
                dst_ref=e.at[pl.ds(5 * k, 5)],
                send_sem=xs.at[k],
                recv_sem=xr.at[k],
                device_id=partner,
                device_id_type=MESH,
            ).wait_recv()
        rows = pl.ds(pl.multiple_of(256 * j, 256), 256)
        block = e[pl.ds(16 * j, 16)].reshape(256, 1024)
        et[:, rows] = block.T
        keys = nn(block, w[0]).astype(BF16)
        values = nn(block, w[1]).astype(BF16)
        v[rows, :] = values
        scores = nt(keys, qc[0]) * (1.0 / 32.0) + st[rows, :]
        st[rows, :] = scores
        slope = nt(values, qc[1])
        gp[rows, :] = slope
        scores = scores.reshape(32, 8, 512)
        peak = jnp.maximum(top, jnp.max(scores, axis=0))
        weights = jnp.exp(scores - peak)
        shrink = jnp.exp(top - peak)
        total = total * shrink + jnp.sum(weights, axis=0)
        dots = dots * shrink + jnp.sum(weights * slope.reshape(32, 8, 512), axis=0)
        return peak, total, dots

    zero = jnp.zeros((8, 512), F32)
    top, total, dots = lax.fori_loop(0, 5, arrive, (jnp.full((8, 512), -1e30, F32), zero, zero))
    peak = jnp.max(top, axis=0, keepdims=True)
    shrink = jnp.exp(top - peak)
    scale = 1.0 / jnp.sum(total * shrink, axis=0, keepdims=True)
    mean = jnp.sum(dots * shrink, axis=0, keepdims=True) * scale

    def normalise(j, carry):
        rows = pl.ds(pl.multiple_of(128 * j, 128), 128)
        probs = jnp.exp(st[rows, :] - peak) * scale
        pg[1, rows, :] = probs.astype(BF16)
        pg[0, rows, :] = (probs * (gp[rows, :] - mean)).astype(BF16)
        return carry

    lax.fori_loop(0, 10, normalise, 0)

    def gather_rows(slot):
        factor = jnp.where(slot == 0, 1.0 / 32.0, 1.0)

        def one(j, carry):
            rows = pl.ds(pl.multiple_of(256 * j, 256), 256)
            a[slot, rows, :] = (nn(et[rows, :], pg[slot]) * factor).astype(BF16)
            return carry

        lax.fori_loop(0, 4, one, 0)

    gather_rows(1 - c)
    operand2 = to_partner(a.at[1 - c], a_in, 1)
    operand2.start()
    sends.append(operand2)
    gather_rows(c)
    operand.wait_recv()
    operand2.wait_recv()

    def hop_copy(g, phase, h, src, dst):
        axis = GROUPS[g][2][phase if phase < 3 else 5 - phase]
        copy = pltpu.make_async_remote_copy(
            src_ref=src, dst_ref=dst, send_sem=gs.at[g, phase, h], recv_sem=gr.at[g, phase, h],
            device_id=along(axis, HOPS[h]), device_id_type=MESH,
        )
        return copy

    def turned(axis, hop, size):
        return pl.multiple_of(((at[axis] + hop) % 4) * size, size)

    copies = {}
    for h in range(4):
        for g, (lo, hi, order) in enumerate(GROUPS):
            hop = HOPS[h] if h < 3 else 0
            rows = pl.ds(turned(order[0], hop, 256), 256)
            term = nn(a[c, rows, :], qc[c, :, lo:hi]) + nn(a_in[rows, :], r_in[:, lo:hi])
            if h < 3:
                snd[h, :, lo:hi] = term.astype(BF16)
                copy = hop_copy(g, 0, h, snd.at[h, :, pl.ds(lo, hi - lo)], rcv.at[h, :, pl.ds(lo, hi - lo)])
                copy.start()
                sends.append(copy)
                copies[g, 0, h] = copy
            else:
                own[:, lo:hi] = term

    for j in range(2):
        ctxb[pl.ds(256 * j, 256), :] = tn(pg[1, :, pl.ds(256 * j, 256)], v[...]).astype(BF16)
    out_ctx = pltpu.make_async_copy(ctxb, ctx, osem.at[0])
    out_ctx.start()

    for phase in (1, 2):
        size = SIZES[phase - 1]
        less = SIZES[phase]
        into, outof = (rcv, rcv2) if phase == 1 else (rcv2, rcv3)
        for g, (lo, hi, order) in enumerate(GROUPS):
            for h in range(3):
                copies[g, phase - 1, h].wait_recv()
            sums = own[0:size, lo:hi]
            for h in range(3):
                sums = sums + into[h, :, lo:hi].astype(F32)
            own[0:size, lo:hi] = sums
            snd[2 + phase, 0:size, lo:hi] = sums.astype(BF16)
            for h in range(3):
                rows = pl.ds(turned(order[phase], HOPS[h], less), less)
                src = snd.at[2 + phase, rows, pl.ds(lo, hi - lo)]
                copy = hop_copy(g, phase, h, src, outof.at[h, :, pl.ds(lo, hi - lo)])
                copy.start()
                sends.append(copy)
                copies[g, phase, h] = copy
            keep = own[pl.ds(turned(order[phase], 0, less), less), lo:hi]
            own[0:less, lo:hi] = keep

    for g, (lo, hi, order) in enumerate(GROUPS):
        for h in range(3):
            copies[g, 2, h].wait_recv()
        sums = own[0:16, lo:hi]
        for h in range(3):
            sums = sums + rcv3[h, :, lo:hi].astype(F32)
        first = at[order[0]] * 256 + at[order[1]] * 64 + at[order[2]] * 16
        res[c, pl.ds(pl.multiple_of(first, 16), 16), lo:hi] = sums.astype(BF16)
    blocks = {}
    for phase in (3, 4, 5):
        depth = 5 - phase
        size = SIZES[depth]
        for g, (lo, hi, order) in enumerate(GROUPS):
            if phase > 3:
                for h in range(3):
                    copies[g, phase - 1, h].wait_recv()
            first = sum(at[order[i]] * SIZES[i] for i in range(depth + 1))
            block = res.at[c, pl.ds(pl.multiple_of(first, size), size), pl.ds(lo, hi - lo)]
            for h in range(3):
                copy = hop_copy(g, phase, h, block, block)
                copy.start()
                sends.append(copy)
                copies[g, phase, h] = copy
    forwards = []
    for h in (3, 1, 2, 0):
        for g, (lo, hi, order) in enumerate(GROUPS):
            hop = HOPS[h] if h < 3 else 0
            if h < 3:
                copies[g, 5, h].wait_recv()
            rows = pl.ds(turned(order[0], 4 - hop, 256), 256)
            block = res.at[c, rows, pl.ds(lo, hi - lo)]
            copy = pltpu.make_async_remote_copy(
                src_ref=block, dst_ref=block, send_sem=fs.at[g, h], recv_sem=fr.at[g, h],
                device_id=partner, device_id_type=MESH,
            )
            copy.start()
            sends.append(copy)
            forwards.append(copy)
    for copy in forwards:
        copy.wait_recv()
    out = pltpu.make_async_copy(res, grads, osem.at[1])
    out.start()
    for copy in sends:
        copy.wait_send()
    out_ctx.wait()
    out.wait()


def body(encoded, queries, cotangent, lengths, key_weight, value_weight):
    any_space = pl.BlockSpec(memory_space=pltpu.HBM)
    dma = pltpu.SemaphoreType.DMA
    grads, context = pl.pallas_call(
        kernel,
        out_shape=(
            jax.ShapeDtypeStruct((2, 1024, 1024), BF16),
            jax.ShapeDtypeStruct((512, 1024), BF16),
        ),
        in_specs=[any_space] * 3 + [pl.BlockSpec(memory_space=pltpu.SMEM)] + [any_space] * 2,
        out_specs=(any_space, any_space),
        scratch_shapes=[
            pltpu.VMEM((80, 16, 1024), BF16),
            pltpu.VMEM((1024, 1280), BF16),
            pltpu.VMEM((1280, 1024), BF16),
            pltpu.VMEM((1280, 512), F32),
            pltpu.VMEM((1280, 512), F32),
            pltpu.VMEM((2, 1280, 512), BF16),
            pltpu.VMEM((2, 512, 1024), BF16),
            pltpu.VMEM((2, 1024, 1024), BF16),
            pltpu.VMEM((2, 1024, 512), BF16),
            pltpu.VMEM((1024, 512), BF16),
            pltpu.VMEM((512, 1024), BF16),
            pltpu.VMEM((256, 1024), F32),
            pltpu.VMEM((5, 256, 1024), BF16),
            pltpu.VMEM((3, 256, 1024), BF16),
            pltpu.VMEM((3, 64, 1024), BF16),
            pltpu.VMEM((3, 16, 1024), BF16),
            pltpu.VMEM((2, 1024, 1024), BF16),
            pltpu.VMEM((512, 1024), BF16),
            dma((5,)), dma((16,)), dma((16,)), dma((2,)), dma((2,)),
            dma((3, 6, 3)), dma((3, 6, 3)), dma((3, 4)), dma((3, 4)), dma((2,)),
        ],
        compiler_params=pltpu.CompilerParams(
            collective_id=0, has_side_effects=True, vmem_limit_bytes=60 * 2**20
        ),
    )(
        jnp.transpose(encoded, (1, 0, 2)),
        queries.reshape(512, 1024),
        cotangent.reshape(512, 1024),
        lengths,
        key_weight,
        value_weight,
    )
    return context.reshape(16, 32, 1024), grads[0].astype(F32), grads[1].astype(F32)


def solution(mesh):
    return jax.shard_map(
        body,
        mesh=mesh,
        in_specs=(
            P("dp", "tm", None),
            P(("dp", "tm"), None, None),
            P(("dp", "tm"), None, None),
            P(("dp", "tm")),
            P(),
            P(),
        ),
        out_specs=(P(("dp", "tm"), None, None), P(), P()),
        check_vma=False,
    )
```

```python
import functools

import jax
import jax.numpy as jnp
from jax import lax
from jax.experimental import pallas as pl
from jax.experimental.pallas import tpu as pltpu
from jax.sharding import PartitionSpec as P

MESH = pl.DeviceIdType.MESH
F32, BF16 = jnp.float32, jnp.bfloat16
OFFS = (
    (0, 0, 0), (0, 0, 1),
    (0, 1, 0), (0, 3, 0), (1, 0, 0), (0, 1, 1), (0, 3, 1), (1, 0, 1),
    (1, 1, 0), (1, 3, 0), (0, 2, 0), (1, 1, 1), (1, 3, 1), (0, 2, 1),
    (1, 2, 0), (1, 2, 1),
)
GROUPS = ((0, 384, (0, 1, 2)), (384, 768, (1, 2, 0)), (768, 1024, (2, 0, 1)))
HOPS = (2, 1, 3)
SIZES = (256, 64, 16)


def nt(a, b):
    return lax.dot_general(a, b, (((1,), (1,)), ((), ())), preferred_element_type=F32)


def nn(a, b):
    return jnp.dot(a, b, preferred_element_type=F32)


def tn(a, b):
    return lax.dot_general(a, b, (((0,), (0,)), ((), ())), preferred_element_type=F32)


def kernel(
    enc, q, cot, lens, wk, wv, res, ctx,
    e, et, v, st, gp, pg, qc, w, a, a_in, r_in, own, snd, rcv, rcv2, rcv3,
    lsem, xs, xr, ds, dr, gs, gr, fs, fr,
):
    tm, dp = lax.axis_index("tm"), lax.axis_index("dp")
    yh, z, c = tm // 8, (tm // 2) % 4, tm % 2
    x, y = dp // 2, yh * 2 + dp % 2
    at = (x, y, z)

    def device(x, y, z, c):
        return ((y // 2) * 8 + z * 2 + c, x * 2 + y % 2)

    def tm_at(off, sign):
        return ((yh + off[0]) % 2) * 8 + ((z + sign * off[1] + 4) % 4) * 2 + (c + off[2]) % 2

    def along(axis, hop):
        there = list(at)
        there[axis] = (there[axis] + hop) % 4
        return device(*there, c)

    partner = device(x, y, z, 1 - c)

    local = [
        pltpu.make_async_copy(q, qc.at[0], lsem.at[0]),
        pltpu.make_async_copy(cot, qc.at[1], lsem.at[1]),
        pltpu.make_async_copy(wk, w.at[0], lsem.at[2]),
        pltpu.make_async_copy(wv, w.at[1], lsem.at[3]),
        pltpu.make_async_copy(
            enc.at[:, pl.ds(pl.multiple_of(16 * tm, 16), 16)], e.at[pl.ds(0, 5)], lsem.at[4]
        ),
    ]
    barrier = pltpu.get_barrier_semaphore()
    peers = [(tm_at(off, 1), dp) for off in OFFS[1:]]
    peers += [along(0, h) for h in (1, 2, 3)] + [along(1, h) for h in (1, 3)]
    for peer in peers:
        pl.semaphore_signal(barrier, inc=1, device_id=peer, device_id_type=MESH)
    for copy in local:
        copy.start()
    pl.semaphore_wait(barrier, len(peers))

    def exchange(k, target):
        return pltpu.make_async_remote_copy(
            src_ref=enc.at[:, pl.ds(pl.multiple_of(16 * target, 16), 16)],
            dst_ref=e.at[pl.ds(5 * k, 5)],
            send_sem=xs.at[k],
            recv_sem=xr.at[k],
            device_id=(target, dp),
            device_id_type=MESH,
        )

    sends = []
    for k, off in enumerate(OFFS):
        if k:
            copy = exchange(k, tm_at(off, 1))
            copy.start()
            sends.append(copy)
    for copy in local[:2]:
        copy.wait()

    def to_partner(src, dst, k):
        return pltpu.make_async_remote_copy(
            src_ref=src, dst_ref=dst, send_sem=ds.at[k], recv_sem=dr.at[k],
            device_id=partner, device_id_type=MESH,
        )

    operand = to_partner(qc.at[1 - c], r_in, 0)
    operand.start()
    sends.append(operand)

    column = lax.broadcasted_iota(jnp.int32, (1, 512), 1) // 32
    limit = jnp.zeros((1, 512), jnp.int32)
    for b in range(16):
        limit = jnp.where(column == b, lens[b], limit)
    row = lax.broadcasted_iota(jnp.int32, (80, 512), 0)
    same = row % 16 == column
    for k, off in enumerate(OFFS):
        position = 5 * tm_at(off, -1) + row // 16
        st[pl.ds(80 * k, 80), :] = jnp.where(same & (position < limit), 0.0, -1e30)

    for copy in local[2:]:
        copy.wait()

    def arrive(j, carry):
        top, total, dots = carry
        for i in range(3):
            k = 3 * j + 1 + i
            pltpu.make_async_remote_copy(
                src_ref=enc.at[:, pl.ds(0, 16)],
                dst_ref=e.at[pl.ds(5 * k, 5)],
                send_sem=xs.at[k],
                recv_sem=xr.at[k],
                device_id=partner,
                device_id_type=MESH,
            ).wait_recv()
        rows = pl.ds(pl.multiple_of(256 * j, 256), 256)
        block = e[pl.ds(16 * j, 16)].reshape(256, 1024)
        et[:, rows] = block.T
        keys = nn(block, w[0]).astype(BF16)
        values = nn(block, w[1]).astype(BF16)
        v[rows, :] = values
        scores = nt(keys, qc[0]) * (1.0 / 32.0) + st[rows, :]
        st[rows, :] = scores
        slope = nt(values, qc[1])
        gp[rows, :] = slope
        scores = scores.reshape(32, 8, 512)
        peak = jnp.maximum(top, jnp.max(scores, axis=0))
        weights = jnp.exp(scores - peak)
        shrink = jnp.exp(top - peak)
        total = total * shrink + jnp.sum(weights, axis=0)
        dots = dots * shrink + jnp.sum(weights * slope.reshape(32, 8, 512), axis=0)
        return peak, total, dots

    zero = jnp.zeros((8, 512), F32)
    top, total, dots = lax.fori_loop(0, 5, arrive, (jnp.full((8, 512), -1e30, F32), zero, zero))
    peak = jnp.max(top, axis=0, keepdims=True)
    shrink = jnp.exp(top - peak)
    scale = 1.0 / jnp.sum(total * shrink, axis=0, keepdims=True)
    mean = jnp.sum(dots * shrink, axis=0, keepdims=True) * scale

    def normalise(j, carry):
        rows = pl.ds(pl.multiple_of(128 * j, 128), 128)
        probs = jnp.exp(st[rows, :] - peak) * scale
        pg[1, rows, :] = probs.astype(BF16)
        pg[0, rows, :] = (probs * (gp[rows, :] - mean)).astype(BF16)
        return carry

    lax.fori_loop(0, 10, normalise, 0)

    def gather_rows(slot):
        factor = jnp.where(slot == 0, 1.0 / 32.0, 1.0)

        def one(j, carry):
            rows = pl.ds(pl.multiple_of(256 * j, 256), 256)
            a[slot, rows, :] = (nn(et[rows, :], pg[slot]) * factor).astype(BF16)
            return carry

        lax.fori_loop(0, 4, one, 0)

    gather_rows(1 - c)
    operand2 = to_partner(a.at[1 - c], a_in, 1)
    operand2.start()
    sends.append(operand2)
    gather_rows(c)
    operand.wait_recv()
    operand2.wait_recv()

    def hop_copy(g, phase, h, src, dst):
        axis = GROUPS[g][2][phase if phase < 3 else 5 - phase]
        copy = pltpu.make_async_remote_copy(
            src_ref=src, dst_ref=dst, send_sem=gs.at[g, phase, h], recv_sem=gr.at[g, phase, h],
            device_id=along(axis, HOPS[h]), device_id_type=MESH,
        )
        return copy

    def turned(axis, hop, size):
        return pl.multiple_of(((at[axis] + hop) % 4) * size, size)

    copies = {}
    for h in range(4):
        for g, (lo, hi, order) in enumerate(GROUPS):
            hop = HOPS[h] if h < 3 else 0
            rows = pl.ds(turned(order[0], hop, 256), 256)
            term = nn(a[c, rows, :], qc[c, :, lo:hi]) + nn(a_in[rows, :], r_in[:, lo:hi])
            if h < 3:
                snd[h, :, lo:hi] = term.astype(BF16)
                copy = hop_copy(g, 0, h, snd.at[h, :, pl.ds(lo, hi - lo)], rcv.at[h, :, pl.ds(lo, hi - lo)])
                copy.start()
                sends.append(copy)
                copies[g, 0, h] = copy
            else:
                own[:, lo:hi] = term

    for j in range(2):
        ctx[pl.ds(256 * j, 256), :] = tn(pg[1, :, pl.ds(256 * j, 256)], v[...]).astype(BF16)

    for phase in (1, 2):
        size = SIZES[phase - 1]
        less = SIZES[phase]
        into, outof = (rcv, rcv2) if phase == 1 else (rcv2, rcv3)
        for g, (lo, hi, order) in enumerate(GROUPS):
            for h in range(3):
                copies[g, phase - 1, h].wait_recv()
            sums = own[0:size, lo:hi]
            for h in range(3):
                sums = sums + into[h, :, lo:hi].astype(F32)
            own[0:size, lo:hi] = sums
            snd[2 + phase, 0:size, lo:hi] = sums.astype(BF16)
            for h in range(3):
                rows = pl.ds(turned(order[phase], HOPS[h], less), less)
                src = snd.at[2 + phase, rows, pl.ds(lo, hi - lo)]
                copy = hop_copy(g, phase, h, src, outof.at[h, :, pl.ds(lo, hi - lo)])
                copy.start()
                sends.append(copy)
                copies[g, phase, h] = copy
            keep = own[pl.ds(turned(order[phase], 0, less), less), lo:hi]
            own[0:less, lo:hi] = keep

    for g, (lo, hi, order) in enumerate(GROUPS):
        for h in range(3):
            copies[g, 2, h].wait_recv()
        sums = own[0:16, lo:hi]
        for h in range(3):
            sums = sums + rcv3[h, :, lo:hi].astype(F32)
        first = at[order[0]] * 256 + at[order[1]] * 64 + at[order[2]] * 16
        res[c, pl.ds(pl.multiple_of(first, 16), 16), lo:hi] = sums.astype(BF16)
    for phase in (3, 4, 5):
        depth = 5 - phase
        size = SIZES[depth]
        for g, (lo, hi, order) in enumerate(GROUPS):
            if phase > 3:
                for h in range(3):
                    copies[g, phase - 1, h].wait_recv()
            first = sum(at[order[i]] * SIZES[i] for i in range(depth + 1))
            block = res.at[c, pl.ds(pl.multiple_of(first, size), size), pl.ds(lo, hi - lo)]
            for h in range(3):
                copy = hop_copy(g, phase, h, block, block)
                copy.start()
                sends.append(copy)
                copies[g, phase, h] = copy
    forwards = []
    for h in (3, 1, 2, 0):
        for g, (lo, hi, order) in enumerate(GROUPS):
            hop = HOPS[h] if h < 3 else 0
            if h < 3:
                copies[g, 5, h].wait_recv()
            rows = pl.ds(turned(order[0], 4 - hop, 256), 256)
            block = res.at[c, rows, pl.ds(lo, hi - lo)]
            copy = pltpu.make_async_remote_copy(
                src_ref=block, dst_ref=block, send_sem=fs.at[g, h], recv_sem=fr.at[g, h],
                device_id=partner, device_id_type=MESH,
            )
            copy.start()
            sends.append(copy)
            forwards.append(copy)
    for copy in forwards:
        copy.wait_recv()
    for copy in sends:
        copy.wait_send()


def finish(sums, context, key_grad, value_grad, context_out, wide, sem):
    copies = [pltpu.make_async_copy(context, context_out, sem.at[8])]
    copies[0].start()
    for i, out in enumerate((key_grad, value_grad)):
        for j in range(4):
            rows = pl.ds(256 * j, 256)
            wide[i, rows, :] = sums[i, rows, :].astype(F32)
            copy = pltpu.make_async_copy(wide.at[i, rows], out.at[rows], sem.at[4 * i + j])
            copy.start()
            copies.append(copy)
    for copy in copies:
        copy.wait()


def body(encoded, queries, cotangent, lengths, key_weight, value_weight):
    any_space = pl.BlockSpec(memory_space=pltpu.HBM)
    dma = pltpu.SemaphoreType.DMA
    grads, context = pl.pallas_call(
        kernel,
        out_shape=(
            pltpu.VMEM((2, 1024, 1024), BF16),
            pltpu.VMEM((512, 1024), BF16),
        ),
        in_specs=[any_space] * 3 + [pl.BlockSpec(memory_space=pltpu.SMEM)] + [any_space] * 2,
        out_specs=(pl.BlockSpec(memory_space=pltpu.VMEM), pl.BlockSpec(memory_space=pltpu.VMEM)),
        scratch_shapes=[
            pltpu.VMEM((80, 16, 1024), BF16),
            pltpu.VMEM((1024, 1280), BF16),
            pltpu.VMEM((1280, 1024), BF16),
            pltpu.VMEM((1280, 512), F32),
            pltpu.VMEM((1280, 512), F32),
            pltpu.VMEM((2, 1280, 512), BF16),
            pltpu.VMEM((2, 512, 1024), BF16),
            pltpu.VMEM((2, 1024, 1024), BF16),
            pltpu.VMEM((2, 1024, 512), BF16),
            pltpu.VMEM((1024, 512), BF16),
            pltpu.VMEM((512, 1024), BF16),
            pltpu.VMEM((256, 1024), F32),
            pltpu.VMEM((5, 256, 1024), BF16),
            pltpu.VMEM((3, 256, 1024), BF16),
            pltpu.VMEM((3, 64, 1024), BF16),
            pltpu.VMEM((3, 16, 1024), BF16),
            dma((5,)), dma((16,)), dma((16,)), dma((2,)), dma((2,)),
            dma((3, 6, 3)), dma((3, 6, 3)), dma((3, 4)), dma((3, 4)),
        ],
        compiler_params=pltpu.CompilerParams(
            collective_id=0, has_side_effects=True, vmem_limit_bytes=50 * 2**20
        ),
    )(
        jnp.transpose(encoded, (1, 0, 2)),
        queries.reshape(512, 1024),
        cotangent.reshape(512, 1024),
        lengths,
        key_weight,
        value_weight,
    )
    key_grad, value_grad, context = pl.pallas_call(
        finish,
        out_shape=(
            jax.ShapeDtypeStruct((1024, 1024), F32),
            jax.ShapeDtypeStruct((1024, 1024), F32),
            jax.ShapeDtypeStruct((512, 1024), BF16),
        ),
        in_specs=[pl.BlockSpec(memory_space=pltpu.VMEM)] * 2,
        out_specs=(any_space,) * 3,
        scratch_shapes=[pltpu.VMEM((2, 1024, 1024), F32), dma((9,))],
        compiler_params=pltpu.CompilerParams(vmem_limit_bytes=16 * 2**20),
    )(grads, context)
    return context.reshape(16, 32, 1024), key_grad, value_grad


def solution(mesh):
    return jax.shard_map(
        body,
        mesh=mesh,
        in_specs=(
            P("dp", "tm", None),
            P(("dp", "tm"), None, None),
            P(("dp", "tm"), None, None),
            P(("dp", "tm")),
            P(),
            P(),
        ),
        out_specs=(P(("dp", "tm"), None, None), P(), P()),
        check_vma=False,
    )
```

```python
import functools

import jax
import jax.numpy as jnp
from jax import lax
from jax.experimental import pallas as pl
from jax.experimental.pallas import tpu as pltpu
from jax.sharding import PartitionSpec as P

MESH = pl.DeviceIdType.MESH
F32, BF16 = jnp.float32, jnp.bfloat16
OFFS = (
    (0, 0, 0), (0, 0, 1),
    (0, 1, 0), (0, 3, 0), (1, 0, 0), (0, 1, 1), (0, 3, 1), (1, 0, 1),
    (1, 1, 0), (1, 3, 0), (0, 2, 0), (1, 1, 1), (1, 3, 1), (0, 2, 1),
    (1, 2, 0), (1, 2, 1),
)
FLOWS = (
    (0, 256, (0, 1, 2)), (256, 384, (1, 2, 0)), (384, 512, (2, 0, 1)),
    (512, 768, (2, 0, 1)), (768, 896, (0, 1, 2)), (896, 1024, (1, 2, 0)),
)
PARTS = ((0, 1, 2), (3, 4, 5))
HOPS = (2, 1, 3)


def nt(a, b):
    return lax.dot_general(a, b, (((1,), (1,)), ((), ())), preferred_element_type=F32)


def nn(a, b):
    return jnp.dot(a, b, preferred_element_type=F32)


def tn(a, b):
    return lax.dot_general(a, b, (((0,), (0,)), ((), ())), preferred_element_type=F32)


def kernel(
    enc, q, cot, lens, wk, wv, res, ctx,
    e, et, v, st, gp, pg, qc, w, a, a_out, r, part, own, snd, snd2, rcv, rcv2, last_sums,
    lsem, xs, xr, ds, dr, gs, gr, fs, fr,
):
    tm, dp = lax.axis_index("tm"), lax.axis_index("dp")
    yh, z, c = tm // 8, (tm // 2) % 4, tm % 2
    x, y = dp // 2, yh * 2 + dp % 2
    at = (x, y, z)

    def device(x, y, z, c):
        return ((y // 2) * 8 + z * 2 + c, x * 2 + y % 2)

    def tm_at(off, sign):
        return ((yh + off[0]) % 2) * 8 + ((z + sign * off[1] + 4) % 4) * 2 + (c + off[2]) % 2

    def along(axis, hop):
        there = list(at)
        there[axis] = (there[axis] + hop) % 4
        return device(*there, c)

    partner = device(x, y, z, 1 - c)

    local = [
        pltpu.make_async_copy(q, qc.at[0], lsem.at[0]),
        pltpu.make_async_copy(cot, qc.at[1], lsem.at[1]),
        pltpu.make_async_copy(wk, w.at[0], lsem.at[2]),
        pltpu.make_async_copy(wv, w.at[1], lsem.at[3]),
        pltpu.make_async_copy(
            enc.at[:, pl.ds(pl.multiple_of(16 * tm, 16), 8)], e.at[0, pl.ds(0, 5)], lsem.at[4]
        ),
        pltpu.make_async_copy(
            enc.at[:, pl.ds(pl.multiple_of(16 * tm + 8, 8), 8)], e.at[1, pl.ds(0, 5)], lsem.at[5]
        ),
    ]
    barrier = pltpu.get_barrier_semaphore()
    peers = [(tm_at(off, 1), dp) for off in OFFS[1:]]
    peers += [along(0, h) for h in (1, 2, 3)] + [along(1, h) for h in (1, 3)]
    for peer in peers:
        pl.semaphore_signal(barrier, inc=1, device_id=peer, device_id_type=MESH)
    for copy in local:
        copy.start()
    pl.semaphore_wait(barrier, len(peers))

    def exchange(h, k, target):
        return pltpu.make_async_remote_copy(
            src_ref=enc.at[:, pl.ds(pl.multiple_of(16 * target + 8 * h, 8), 8)],
            dst_ref=e.at[h, pl.ds(5 * k, 5)],
            send_sem=xs.at[h, k],
            recv_sem=xr.at[h, k],
            device_id=(target, dp),
            device_id_type=MESH,
        )

    sends = []
    for h in range(2):
        for k, off in enumerate(OFFS):
            if k:
                copy = exchange(h, k, tm_at(off, 1))
                copy.start()
                sends.append(copy)
    for copy in local[:2]:
        copy.wait()

    def to_partner(src, dst, k):
        return pltpu.make_async_remote_copy(
            src_ref=src, dst_ref=dst, send_sem=ds.at[k], recv_sem=dr.at[k],
            device_id=partner, device_id_type=MESH,
        )

    operands = []
    for h in range(2):
        half = pl.ds(256 * h, 256)
        copy = to_partner(qc.at[1 - c, half], r.at[h, pl.ds(256, 256)], h)
        copy.start()
        sends.append(copy)
        operands.append(copy)
        copy = pltpu.make_async_copy(qc.at[c, half], r.at[h, pl.ds(0, 256)], lsem.at[6 + h])
        copy.start()
        local.append(copy)

    column = lax.broadcasted_iota(jnp.int32, (1, 256), 1) // 32
    row = lax.broadcasted_iota(jnp.int32, (40, 256), 0)
    same = row % 8 == column
    for h in range(2):
        limit = jnp.zeros((1, 256), jnp.int32)
        for b in range(8):
            limit = jnp.where(column == b, lens[8 * h + b], limit)
        for k, off in enumerate(OFFS):
            position = 5 * tm_at(off, -1) + row // 8
            st[h, pl.ds(40 * k, 40), :] = jnp.where(same & (position < limit), 0.0, -1e30)

    for copy in local[2:]:
        copy.wait()

    def stream(h):
        def arrive(j, carry):
            top, total, dots = carry
            for i in range(3):
                k = 3 * j + 1 + i
                pltpu.make_async_remote_copy(
                    src_ref=enc.at[:, pl.ds(0, 8)],
                    dst_ref=e.at[h, pl.ds(5 * k, 5)],
                    send_sem=xs.at[h, k],
                    recv_sem=xr.at[h, k],
                    device_id=partner,
                    device_id_type=MESH,
                ).wait_recv()
            rows = pl.ds(pl.multiple_of(128 * j, 128), 128)
            block = e[h, pl.ds(16 * j, 16)].reshape(128, 1024)
            et[h, :, rows] = block.T
            keys = nn(block, w[0]).astype(BF16)
            values = nn(block, w[1]).astype(BF16)
            v[h, rows, :] = values
            scores = nt(keys, qc[0, pl.ds(256 * h, 256)]) * (1.0 / 32.0) + st[h, rows, :]
            st[h, rows, :] = scores
            slope = nt(values, qc[1, pl.ds(256 * h, 256)])
            gp[h, rows, :] = slope
            scores = scores.reshape(16, 8, 256)
            peak = jnp.maximum(top, jnp.max(scores, axis=0))
            weights = jnp.exp(scores - peak)
            shrink = jnp.exp(top - peak)
            total = total * shrink + jnp.sum(weights, axis=0)
            dots = dots * shrink + jnp.sum(weights * slope.reshape(16, 8, 256), axis=0)
            return peak, total, dots

        zero = jnp.zeros((8, 256), F32)
        top, total, dots = lax.fori_loop(0, 5, arrive, (jnp.full((8, 256), -1e30, F32), zero, zero))
        peak = jnp.max(top, axis=0, keepdims=True)
        shrink = jnp.exp(top - peak)
        scale = 1.0 / jnp.sum(total * shrink, axis=0, keepdims=True)
        mean = jnp.sum(dots * shrink, axis=0, keepdims=True) * scale

        def normalise(j, carry):
            rows = pl.ds(pl.multiple_of(128 * j, 128), 128)
            probs = jnp.exp(st[h, rows, :] - peak) * scale
            pg[h, 1, rows, :] = probs.astype(BF16)
            pg[h, 0, rows, :] = (probs * (gp[h, rows, :] - mean)).astype(BF16)
            return carry

        lax.fori_loop(0, 5, normalise, 0)

    def weigh(h, slot):
        factor = jnp.where(slot == 0, 1.0 / 32.0, 1.0)
        return (nn(et[h], pg[h, slot]) * factor).astype(BF16)

    def swap(h):
        a_out[h] = weigh(h, 1 - c)
        copy = to_partner(a_out.at[h], a.at[h, :, pl.ds(256, 256)], 2 + h)
        copy.start()
        sends.append(copy)
        a[h, :, 0:256] = weigh(h, c)
        operands[h].wait_recv()
        return copy

    stream(0)
    swap(0).wait_recv()
    def first_half(j, carry):
        rows = pl.ds(pl.multiple_of(256 * j, 256), 256)
        part[rows, :] = nn(a[0, rows, :], r[0])
        return carry

    lax.fori_loop(0, 4, first_half, 0)
    stream(1)
    last = swap(1)
    last.wait_recv()

    def pick(axis, value):
        return value[axis] * (1 - c) + value[(axis + 1) % 3] * c

    def there(axis, hop):
        place = [
            (at[i] + hop * ((1 - c) if i == axis else c if i == (axis + 1) % 3 else 0)) % 4
            for i in range(3)
        ]
        return device(*place, c)

    copies = {}

    def hop_copy(f, phase, h, axis, src, dst):
        copy = pltpu.make_async_remote_copy(
            src_ref=src, dst_ref=dst, send_sem=gs.at[f, phase, h], recv_sem=gr.at[f, phase, h],
            device_id=there(axis, HOPS[h]), device_id_type=MESH,
        )
        copy.start()
        sends.append(copy)
        copies[f, phase, h] = copy

    def arrived(f, phase):
        for h in range(3):
            copies[f, phase, h].wait_recv()

    def turned(axis, hop, size):
        return pl.multiple_of(((pick(axis, at) + hop) % 4) * size, size)

    for flows in PARTS:
        lo, hi = FLOWS[flows[0]][0], FLOWS[flows[-1]][1]

        def second_half(j, carry):
            rows = pl.ds(pl.multiple_of(256 * j, 256), 256)
            term = part[rows, lo:hi] + nn(a[1, rows, :], r[1, :, lo:hi])
            part[rows, lo:hi] = term
            snd[rows, lo:hi] = term.astype(BF16)
            return carry

        lax.fori_loop(0, 4, second_half, 0)
        for h in range(3):
            for f in flows:
                lo, hi, order = FLOWS[f]
                cols = pl.ds(lo, hi - lo)
                src = snd.at[pl.ds(turned(order[0], HOPS[h], 256), 256), cols]
                hop_copy(f, 0, h, order[0], src, rcv.at[h, :, cols])

    for h in range(2):
        ctx[pl.ds(256 * h, 256), :] = tn(pg[h, 1], v[h]).astype(BF16)

    for flows in PARTS:
        for f in flows:
            lo, hi, order = FLOWS[f]
            cols = pl.ds(lo, hi - lo)
            arrived(f, 0)
            sums = part[pl.ds(turned(order[0], 0, 256), 256), lo:hi]
            for h in range(3):
                sums = sums + rcv[h, :, lo:hi].astype(F32)
            own[:, lo:hi] = sums
            snd2[:, lo:hi] = sums.astype(BF16)
            for h in range(3):
                src = snd2.at[pl.ds(turned(order[1], HOPS[h], 64), 64), cols]
                hop_copy(f, 1, h, order[1], src, rcv2.at[h, :, cols])

    for flows in PARTS:
        for f in flows:
            lo, hi, order = FLOWS[f]
            cols = pl.ds(lo, hi - lo)
            arrived(f, 1)
            sums = own[pl.ds(turned(order[1], 0, 64), 64), lo:hi]
            for h in range(3):
                sums = sums + rcv2[h, :, lo:hi].astype(F32)
            mine = pick(order[2], at)
            last_sums[mine, :, lo:hi] = sums.astype(BF16)
            block = last_sums.at[mine, :, cols]
            for h in range(3):
                hop_copy(f, 2, h, order[2], block, block)

    for flows in PARTS:
        for f in flows:
            lo, hi, order = FLOWS[f]
            arrived(f, 2)
            sums = last_sums[0, :, lo:hi].astype(F32)
            for i in range(1, 4):
                sums = sums + last_sums[i, :, lo:hi].astype(F32)
            first = pick(order[0], at) * 256 + pick(order[1], at) * 64
            rows = pl.ds(pl.multiple_of(first, 64), 64)
            res[c, rows, lo:hi] = sums.astype(BF16)
            block = res.at[c, rows, pl.ds(lo, hi - lo)]
            for h in range(3):
                hop_copy(f, 3, h, order[1], block, block)

    for flows in PARTS:
        for f in flows:
            lo, hi, order = FLOWS[f]
            arrived(f, 3)
            block = res.at[c, pl.ds(turned(order[0], 0, 256), 256), pl.ds(lo, hi - lo)]
            for h in range(3):
                hop_copy(f, 4, h, order[0], block, block)

    forwards = []
    for flows in PARTS:
        for h in (3, 1, 2, 0):
            for f in flows:
                lo, hi, order = FLOWS[f]
                hop = 0
                if h < 3:
                    hop = HOPS[h]
                    copies[f, 4, h].wait_recv()
                block = res.at[c, pl.ds(turned(order[0], 4 - hop, 256), 256), pl.ds(lo, hi - lo)]
                copy = pltpu.make_async_remote_copy(
                    src_ref=block, dst_ref=block, send_sem=fs.at[f, h], recv_sem=fr.at[f, h],
                    device_id=partner, device_id_type=MESH,
                )
                copy.start()
                sends.append(copy)
                forwards.append(copy)
    for copy in forwards:
        copy.wait_recv()
    for copy in sends:
        copy.wait_send()


def finish(sums, context, key_grad, value_grad, context_out, wide, sem):
    copies = [pltpu.make_async_copy(context, context_out, sem.at[8])]
    copies[0].start()
    for i, out in enumerate((key_grad, value_grad)):
        for j in range(4):
            rows = pl.ds(256 * j, 256)
            wide[i, rows, :] = sums[i, rows, :].astype(F32)
            copy = pltpu.make_async_copy(wide.at[i, rows], out.at[rows], sem.at[4 * i + j])
            copy.start()
            copies.append(copy)
    for copy in copies:
        copy.wait()


def body(encoded, queries, cotangent, lengths, key_weight, value_weight):
    any_space = pl.BlockSpec(memory_space=pltpu.HBM)
    dma = pltpu.SemaphoreType.DMA
    grads, context = pl.pallas_call(
        kernel,
        out_shape=(
            pltpu.VMEM((2, 1024, 1024), BF16),
            pltpu.VMEM((512, 1024), BF16),
        ),
        in_specs=[any_space] * 3 + [pl.BlockSpec(memory_space=pltpu.SMEM)] + [any_space] * 2,
        out_specs=(pl.BlockSpec(memory_space=pltpu.VMEM), pl.BlockSpec(memory_space=pltpu.VMEM)),
        scratch_shapes=[
            pltpu.VMEM((2, 80, 8, 1024), BF16),
            pltpu.VMEM((2, 1024, 640), BF16),
            pltpu.VMEM((2, 640, 1024), BF16),
            pltpu.VMEM((2, 640, 256), F32),
            pltpu.VMEM((2, 640, 256), F32),
            pltpu.VMEM((2, 2, 640, 256), BF16),
            pltpu.VMEM((2, 512, 1024), BF16),
            pltpu.VMEM((2, 1024, 1024), BF16),
            pltpu.VMEM((2, 1024, 512), BF16),
            pltpu.VMEM((2, 1024, 256), BF16),
            pltpu.VMEM((2, 512, 1024), BF16),
            pltpu.VMEM((1024, 1024), F32),
            pltpu.VMEM((256, 1024), F32),
            pltpu.VMEM((1024, 1024), BF16),
            pltpu.VMEM((256, 1024), BF16),
            pltpu.VMEM((3, 256, 1024), BF16),
            pltpu.VMEM((3, 64, 1024), BF16),
            pltpu.VMEM((4, 64, 1024), BF16),
            dma((8,)), dma((2, 16)), dma((2, 16)), dma((4,)), dma((4,)),
            dma((6, 5, 3)), dma((6, 5, 3)), dma((6, 4)), dma((6, 4)),
        ],
        compiler_params=pltpu.CompilerParams(
            collective_id=0, has_side_effects=True, vmem_limit_bytes=50 * 2**20
        ),
    )(
        jnp.transpose(encoded, (1, 0, 2)),
        queries.reshape(512, 1024),
        cotangent.reshape(512, 1024),
        lengths,
        key_weight,
        value_weight,
    )
    key_grad, value_grad, context = pl.pallas_call(
        finish,
        out_shape=(
            jax.ShapeDtypeStruct((1024, 1024), F32),
            jax.ShapeDtypeStruct((1024, 1024), F32),
            jax.ShapeDtypeStruct((512, 1024), BF16),
        ),
        in_specs=[pl.BlockSpec(memory_space=pltpu.VMEM)] * 2,
        out_specs=(any_space,) * 3,
        scratch_shapes=[pltpu.VMEM((2, 1024, 1024), F32), dma((9,))],
        compiler_params=pltpu.CompilerParams(vmem_limit_bytes=16 * 2**20),
    )(grads, context)
    return context.reshape(16, 32, 1024), key_grad, value_grad


def solution(mesh):
    return jax.shard_map(
        body,
        mesh=mesh,
        in_specs=(
            P("dp", "tm", None),
            P(("dp", "tm"), None, None),
            P(("dp", "tm"), None, None),
            P(("dp", "tm")),
            P(),
            P(),
        ),
        out_specs=(P(("dp", "tm"), None, None), P(), P()),
        check_vma=False,
    )
```

```python
import functools

import jax
import jax.numpy as jnp
from jax import lax
from jax.experimental import pallas as pl
from jax.experimental.pallas import tpu as pltpu
from jax.sharding import PartitionSpec as P

MESH = pl.DeviceIdType.MESH
F32, BF16 = jnp.float32, jnp.bfloat16
OFFS = (
    (0, 0, 0), (0, 0, 1),
    (0, 1, 0), (0, 3, 0), (1, 0, 0), (0, 1, 1), (0, 3, 1), (1, 0, 1),
    (1, 1, 0), (1, 3, 0), (0, 2, 0), (1, 1, 1), (1, 3, 1), (0, 2, 1),
    (1, 2, 0), (1, 2, 1),
)
FLOWS = (
    (0, 128, (0, 1, 2), 0, 256), (128, 256, (1, 2, 0), 0, 256),
    (256, 384, (2, 0, 1), 0, 256), (384, 512, (0, 1, 2), 0, 256),
    (512, 640, (1, 2, 0), 0, 256), (640, 768, (2, 0, 1), 0, 256),
    (768, 896, (0, 1, 2), 0, 256),
    (896, 1024, (1, 2, 0), 0, 128), (896, 1024, (2, 0, 1), 512, 128),
)
PARTS = ((0, 1), (2, 3), (4, 5), (6, 7, 8))
HOPS = (2, 1, 3)
BACK = (0, 1, 2)
TALL = 1024
SCHEDULE = ((0, 0), (0, 1), (0, 2), (0, 3), (6, 0)) + tuple((s, p) for s in range(1, 6) for p in range(4))


def nt(a, b):
    return lax.dot_general(a, b, (((1,), (1,)), ((), ())), preferred_element_type=F32)


def nn(a, b):
    return jnp.dot(a, b, preferred_element_type=F32)


def tn(a, b):
    return lax.dot_general(a, b, (((0,), (0,)), ((), ())), preferred_element_type=F32)


def kernel(
    enc, q, cot, lens, wk, wv, res, ctx,
    e, et, v, st, gp, pg, qc, w, a, a_out, r, part, own, snd, snd2, rcv, rcv2, last_sums,
    lsem, xs, xr, ds, dr, gs, gr, fs, fr,
):
    tm, dp = lax.axis_index("tm"), lax.axis_index("dp")
    yh, z, c = tm // 8, (tm // 2) % 4, tm % 2
    x, y = dp // 2, yh * 2 + dp % 2
    at = (x, y, z)

    def device(x, y, z, c):
        return ((y // 2) * 8 + z * 2 + c, x * 2 + y % 2)

    def tm_at(off, sign):
        return ((yh + off[0]) % 2) * 8 + ((z + sign * off[1] + 4) % 4) * 2 + (c + off[2]) % 2

    def along(axis, hop):
        there = list(at)
        there[axis] = (there[axis] + hop) % 4
        return device(*there, c)

    partner = device(x, y, z, 1 - c)

    local = [
        pltpu.make_async_copy(q, qc.at[0], lsem.at[0]),
        pltpu.make_async_copy(cot, qc.at[1], lsem.at[1]),
        pltpu.make_async_copy(wk, w.at[0], lsem.at[2]),
        pltpu.make_async_copy(wv, w.at[1], lsem.at[3]),
        pltpu.make_async_copy(
            enc.at[:, pl.ds(pl.multiple_of(16 * tm, 16), 8)], e.at[0, pl.ds(0, 5)], lsem.at[4]
        ),
        pltpu.make_async_copy(
            enc.at[:, pl.ds(pl.multiple_of(16 * tm + 8, 8), 8)], e.at[1, pl.ds(0, 5)], lsem.at[5]
        ),
    ]
    barrier = pltpu.get_barrier_semaphore()
    peers = [(tm_at(off, 1), dp) for off in OFFS[1:]]
    peers += [along(0, h) for h in (1, 2, 3)] + [along(1, h) for h in (1, 3)]
    for peer in peers:
        pl.semaphore_signal(barrier, inc=1, device_id=peer, device_id_type=MESH)
    for copy in local:
        copy.start()
    pl.semaphore_wait(barrier, len(peers))

    def exchange(h, k, target):
        return pltpu.make_async_remote_copy(
            src_ref=enc.at[:, pl.ds(pl.multiple_of(16 * target + 8 * h, 8), 8)],
            dst_ref=e.at[h, pl.ds(5 * k, 5)],
            send_sem=xs.at[h, k],
            recv_sem=xr.at[h, k],
            device_id=(target, dp),
            device_id_type=MESH,
        )

    sends = []
    for h in range(2):
        for k, off in enumerate(OFFS):
            if k:
                copy = exchange(h, k, tm_at(off, 1))
                copy.start()
                sends.append(copy)
    for copy in local[:2]:
        copy.wait()

    def to_partner(src, dst, k):
        return pltpu.make_async_remote_copy(
            src_ref=src, dst_ref=dst, send_sem=ds.at[k], recv_sem=dr.at[k],
            device_id=partner, device_id_type=MESH,
        )

    operands = []
    for h in range(2):
        half = pl.ds(256 * h, 256)
        copy = to_partner(qc.at[1 - c, half], r.at[h, pl.ds(256, 256)], h)
        copy.start()
        sends.append(copy)
        operands.append(copy)
        copy = pltpu.make_async_copy(qc.at[c, half], r.at[h, pl.ds(0, 256)], lsem.at[6 + h])
        copy.start()
        local.append(copy)

    column = lax.broadcasted_iota(jnp.int32, (1, 256), 1) // 32
    row = lax.broadcasted_iota(jnp.int32, (40, 256), 0)
    same = row % 8 == column
    for h in range(2):
        limit = jnp.zeros((1, 256), jnp.int32)
        for b in range(8):
            limit = jnp.where(column == b, lens[8 * h + b], limit)
        for k, off in enumerate(OFFS):
            position = 5 * tm_at(off, -1) + row // 8
            st[h, pl.ds(40 * k, 40), :] = jnp.where(same & (position < limit), 0.0, -1e30)

    for copy in local[2:]:
        copy.wait()

    def stream(h):
        def arrive(j, carry):
            top, total, dots = carry
            for i in range(3):
                k = 3 * j + 1 + i
                pltpu.make_async_remote_copy(
                    src_ref=enc.at[:, pl.ds(0, 8)],
                    dst_ref=e.at[h, pl.ds(5 * k, 5)],
                    send_sem=xs.at[h, k],
                    recv_sem=xr.at[h, k],
                    device_id=partner,
                    device_id_type=MESH,
                ).wait_recv()
            rows = pl.ds(pl.multiple_of(128 * j, 128), 128)
            block = e[h, pl.ds(16 * j, 16)].reshape(128, 1024)
            et[h, :, rows] = block.T
            keys = nn(block, w[0]).astype(BF16)
            values = nn(block, w[1]).astype(BF16)
            v[h, rows, :] = values
            scores = nt(keys, qc[0, pl.ds(256 * h, 256)]) * (1.0 / 32.0) + st[h, rows, :]
            st[h, rows, :] = scores
            slope = nt(values, qc[1, pl.ds(256 * h, 256)])
            gp[h, rows, :] = slope
            scores = scores.reshape(16, 8, 256)
            peak = jnp.maximum(top, jnp.max(scores, axis=0))
            weights = jnp.exp(scores - peak)
            shrink = jnp.exp(top - peak)
            total = total * shrink + jnp.sum(weights, axis=0)
            dots = dots * shrink + jnp.sum(weights * slope.reshape(16, 8, 256), axis=0)
            return peak, total, dots

        zero = jnp.zeros((8, 256), F32)
        top, total, dots = lax.fori_loop(0, 5, arrive, (jnp.full((8, 256), -1e30, F32), zero, zero))
        peak = jnp.max(top, axis=0, keepdims=True)
        shrink = jnp.exp(top - peak)
        scale = 1.0 / jnp.sum(total * shrink, axis=0, keepdims=True)
        mean = jnp.sum(dots * shrink, axis=0, keepdims=True) * scale

        def normalise(j, carry):
            rows = pl.ds(pl.multiple_of(128 * j, 128), 128)
            probs = jnp.exp(st[h, rows, :] - peak) * scale
            pg[h, 1, rows, :] = probs.astype(BF16)
            pg[h, 0, rows, :] = (probs * (gp[h, rows, :] - mean)).astype(BF16)
            return carry

        lax.fori_loop(0, 5, normalise, 0)

    def weigh(h, slot, rows):
        factor = jnp.where(slot == 0, 1.0 / 32.0, 1.0)
        return (nn(et[h, rows, :], pg[h, slot]) * factor).astype(BF16)

    def swap(h):
        swapped = []
        for i in range(2):
            rows = pl.ds(512 * i, 512)
            a_out[h, rows, :] = weigh(h, 1 - c, rows)
            copy = to_partner(a_out.at[h, rows], a.at[h, rows, pl.ds(256, 256)], 2 + 2 * h + i)
            copy.start()
            sends.append(copy)
            swapped.append(copy)
        a[h, :, 0:256] = weigh(h, c, pl.ds(0, 1024))
        swapped.append(operands[h])
        return swapped

    stream(0)
    for copy in swap(0):
        copy.wait_recv()
    def first_half(j, carry):
        rows = pl.ds(pl.multiple_of(256 * j, 256), 256)
        part[rows, :] = nn(a[0, rows, :], r[0])
        return carry

    lax.fori_loop(0, 4, first_half, 0)
    stream(1)
    last = swap(1)
    for copy in last:
        copy.wait_recv()

    def pick(axis, value):
        return value[axis] * (1 - c) + value[(axis + 1) % 3] * c

    def there(axis, hop):
        place = [
            (at[i] + hop * ((1 - c) if i == axis else c if i == (axis + 1) % 3 else 0)) % 4
            for i in range(3)
        ]
        return device(*place, c)

    copies = {}

    def hop_copy(f, phase, h, axis, src, dst):
        copy = pltpu.make_async_remote_copy(
            src_ref=src, dst_ref=dst, send_sem=gs.at[f, phase, h], recv_sem=gr.at[f, phase, h],
            device_id=there(axis, HOPS[h]), device_id_type=MESH,
        )
        copy.start()
        sends.append(copy)
        copies[f, phase, h] = copy

    def arrived(f, phase):
        for h in range(3):
            copies[f, phase, h].wait_recv()

    def turned(axis, hop, size, start=0):
        return pl.multiple_of(start + ((pick(axis, at) + hop) % 4) * size, size)

    forwards = []

    def own_terms(flows):
        first, last = FLOWS[flows[0]][0], FLOWS[flows[-1]][1]

        def second_half(j, carry):
            rows = pl.ds(pl.multiple_of(TALL * j, TALL), TALL)
            term = part[rows, first:last] + nn(a[1, rows, :], r[1, :, first:last])
            part[rows, first:last] = term
            snd[rows, first:last] = term.astype(BF16)
            return carry

        lax.fori_loop(0, 1024 // TALL, second_half, 0)
        for h in range(3):
            for f in flows:
                lo, hi, order, start, size = FLOWS[f]
                cols = pl.ds(lo, hi - lo)
                src = snd.at[pl.ds(turned(order[0], HOPS[h], size, start), size), cols]
                hop_copy(f, 0, h, order[0], src, rcv.at[h, pl.ds(start // 4, size), cols])

    def second_axis(flows):
        for f in flows:
            lo, hi, order, start, size = FLOWS[f]
            cols = pl.ds(lo, hi - lo)
            base, less = start // 4, size // 4
            arrived(f, 0)
            sums = part[pl.ds(turned(order[0], 0, size, start), size), lo:hi]
            for h in range(3):
                sums = sums + rcv[h, base : base + size, lo:hi].astype(F32)
            own[base : base + size, lo:hi] = sums
            snd2[base : base + size, lo:hi] = sums.astype(BF16)
            for h in range(3):
                src = snd2.at[pl.ds(turned(order[1], HOPS[h], less, base), less), cols]
                hop_copy(f, 1, h, order[1], src, rcv2.at[h, pl.ds(start // 16, less), cols])

    def third_axis(flows):
        for f in flows:
            lo, hi, order, start, size = FLOWS[f]
            base, less = start // 16, size // 4
            arrived(f, 1)
            sums = own[pl.ds(turned(order[1], 0, less, start // 4), less), lo:hi]
            for h in range(3):
                sums = sums + rcv2[h, base : base + less, lo:hi].astype(F32)
            mine = pick(order[2], at)
            last_sums[mine, base : base + less, lo:hi] = sums.astype(BF16)
            block = last_sums.at[mine, pl.ds(base, less), pl.ds(lo, hi - lo)]
            for h in range(3):
                hop_copy(f, 2, h, order[2], block, block)

    def back_second(flows):
        for f in flows:
            lo, hi, order, start, size = FLOWS[f]
            base, less = start // 16, size // 4
            arrived(f, 2)
            sums = last_sums[0, base : base + less, lo:hi].astype(F32)
            for i in range(1, 4):
                sums = sums + last_sums[i, base : base + less, lo:hi].astype(F32)
            first = start + pick(order[0], at) * size + pick(order[1], at) * less
            rows = pl.ds(pl.multiple_of(first, less), less)
            res[c, rows, lo:hi] = sums.astype(BF16)
            block = res.at[c, rows, pl.ds(lo, hi - lo)]
            for h in range(3):
                hop_copy(f, 3, h, order[1], block, block)

    def gathered(f, hop):
        lo, hi, order, start, size = FLOWS[f]
        return res.at[c, pl.ds(turned(order[0], hop, size, start), size), pl.ds(lo, hi - lo)]

    def forward(f, h):
        block = gathered(f, 4 - HOPS[h] if h < 3 else 0)
        copy = pltpu.make_async_remote_copy(
            src_ref=block, dst_ref=block, send_sem=fs.at[f, h], recv_sem=fr.at[f, h],
            device_id=partner, device_id_type=MESH,
        )
        copy.start()
        sends.append(copy)
        forwards.append(copy)

    def back_first(flows):
        for f in flows:
            arrived(f, 3)
            block = gathered(f, 0)
            for h in BACK:
                hop_copy(f, 4, h, FLOWS[f][2][0], block, block)
        for f in flows:
            forward(f, 3)

    def to_other_core(flows):
        for h in BACK:
            for f in flows:
                copies[f, 4, h].wait_recv()
                forward(f, h)

    def contexts(flows):
        for h in range(2):
            ctx[pl.ds(256 * h, 256), :] = tn(pg[h, 1], v[h]).astype(BF16)

    steps = (own_terms, second_axis, third_axis, back_second, back_first, to_other_core, contexts)
    for step, p in SCHEDULE:
        with jax.named_scope(f"s{step}_{p}"):
            steps[step](PARTS[p])
    for copy in forwards:
        copy.wait_recv()
    for copy in sends:
        copy.wait_send()


def finish(sums, context, key_grad, value_grad, context_out, wide, sem):
    copies = [pltpu.make_async_copy(context, context_out, sem.at[8])]
    copies[0].start()
    for i, out in enumerate((key_grad, value_grad)):
        for j in range(4):
            rows = pl.ds(256 * j, 256)
            wide[i, rows, :] = sums[i, rows, :].astype(F32)
            copy = pltpu.make_async_copy(wide.at[i, rows], out.at[rows], sem.at[4 * i + j])
            copy.start()
            copies.append(copy)
    for copy in copies:
        copy.wait()


def body(encoded, queries, cotangent, lengths, key_weight, value_weight):
    any_space = pl.BlockSpec(memory_space=pltpu.HBM)
    dma = pltpu.SemaphoreType.DMA
    grads, context = pl.pallas_call(
        kernel,
        out_shape=(
            pltpu.VMEM((2, 1024, 1024), BF16),
            pltpu.VMEM((512, 1024), BF16),
        ),
        in_specs=[any_space] * 3 + [pl.BlockSpec(memory_space=pltpu.SMEM)] + [any_space] * 2,
        out_specs=(pl.BlockSpec(memory_space=pltpu.VMEM), pl.BlockSpec(memory_space=pltpu.VMEM)),
        scratch_shapes=[
            pltpu.VMEM((2, 80, 8, 1024), BF16),
            pltpu.VMEM((2, 1024, 640), BF16),
            pltpu.VMEM((2, 640, 1024), BF16),
            pltpu.VMEM((2, 640, 256), F32),
            pltpu.VMEM((2, 640, 256), F32),
            pltpu.VMEM((2, 2, 640, 256), BF16),
            pltpu.VMEM((2, 512, 1024), BF16),
            pltpu.VMEM((2, 1024, 1024), BF16),
            pltpu.VMEM((2, 1024, 512), BF16),
            pltpu.VMEM((2, 1024, 256), BF16),
            pltpu.VMEM((2, 512, 1024), BF16),
            pltpu.VMEM((1024, 1024), F32),
            pltpu.VMEM((256, 1024), F32),
            pltpu.VMEM((1024, 1024), BF16),
            pltpu.VMEM((256, 1024), BF16),
            pltpu.VMEM((3, 256, 1024), BF16),
            pltpu.VMEM((3, 64, 1024), BF16),
            pltpu.VMEM((4, 64, 1024), BF16),
            dma((8,)), dma((2, 16)), dma((2, 16)), dma((6,)), dma((6,)),
            dma((9, 5, 3)), dma((9, 5, 3)), dma((9, 4)), dma((9, 4)),
        ],
        compiler_params=pltpu.CompilerParams(
            collective_id=0, has_side_effects=True, vmem_limit_bytes=50 * 2**20
        ),
    )(
        jnp.transpose(encoded, (1, 0, 2)),
        queries.reshape(512, 1024),
        cotangent.reshape(512, 1024),
        lengths,
        key_weight,
        value_weight,
    )
    key_grad, value_grad, context = pl.pallas_call(
        finish,
        out_shape=(
            jax.ShapeDtypeStruct((1024, 1024), F32),
            jax.ShapeDtypeStruct((1024, 1024), F32),
            jax.ShapeDtypeStruct((512, 1024), BF16),
        ),
        in_specs=[pl.BlockSpec(memory_space=pltpu.VMEM)] * 2,
        out_specs=(any_space,) * 3,
        scratch_shapes=[pltpu.VMEM((2, 1024, 1024), F32), dma((9,))],
        compiler_params=pltpu.CompilerParams(vmem_limit_bytes=16 * 2**20),
    )(grads, context)
    return context.reshape(16, 32, 1024), key_grad, value_grad


def solution(mesh):
    return jax.shard_map(
        body,
        mesh=mesh,
        in_specs=(
            P("dp", "tm", None),
            P(("dp", "tm"), None, None),
            P(("dp", "tm"), None, None),
            P(("dp", "tm")),
            P(),
            P(),
        ),
        out_specs=(P(("dp", "tm"), None, None), P(), P()),
        check_vma=False,
    )
```

```python
import functools

import jax
import jax.numpy as jnp
from jax import lax
from jax.experimental import pallas as pl
from jax.experimental.pallas import tpu as pltpu
from jax.sharding import PartitionSpec as P

MESH = pl.DeviceIdType.MESH
F32, BF16 = jnp.float32, jnp.bfloat16
OFFS = (
    (0, 0, 0), (0, 0, 1),
    (0, 1, 0), (0, 3, 0), (1, 0, 0), (0, 1, 1), (0, 3, 1), (1, 0, 1),
    (1, 1, 0), (1, 3, 0), (0, 2, 0), (1, 1, 1), (1, 3, 1), (0, 2, 1),
    (1, 2, 0), (1, 2, 1),
)
FLOWS = (
    (0, 128, (0, 1, 2), 0, 256), (128, 256, (1, 2, 0), 0, 256),
    (256, 384, (2, 0, 1), 0, 256), (384, 512, (0, 1, 2), 0, 256),
    (512, 640, (1, 2, 0), 0, 256), (640, 768, (2, 0, 1), 0, 256),
    (768, 896, (0, 1, 2), 0, 256),
    (896, 1024, (1, 2, 0), 0, 128), (896, 1024, (2, 0, 1), 512, 128),
)
PARTS = ((0, 1), (2, 3), (4, 5), (6, 7, 8))
HOPS = (2, 1, 3)
BACK = (0, 1, 2)
TALL = 1024
SCHEDULE = ((0, 0), (0, 1), (0, 2), (0, 3), (6, 0), (7, 0)) + tuple((s, p) for s in range(1, 5) for p in range(4)) + (
    (7, 0), (5, 0), (5, 1), (5, 2), (5, 3),
)


def nt(a, b):
    return lax.dot_general(a, b, (((1,), (1,)), ((), ())), preferred_element_type=F32)


def nn(a, b):
    return jnp.dot(a, b, preferred_element_type=F32)


def tn(a, b):
    return lax.dot_general(a, b, (((0,), (0,)), ((), ())), preferred_element_type=F32)


def kernel(
    enc, q, cot, lens, wk, wv, res, ctx,
    e, et, v, st, gp, pg, qc, w, a, a_out, r, part, own, snd, snd2, rcv, rcv2, last_sums,
    lsem, xs, xr, ds, dr, gs, gr, fs, fr,
):
    tm, dp = lax.axis_index("tm"), lax.axis_index("dp")
    yh, z, c = tm // 8, (tm // 2) % 4, tm % 2
    x, y = dp // 2, yh * 2 + dp % 2
    at = (x, y, z)

    def device(x, y, z, c):
        return ((y // 2) * 8 + z * 2 + c, x * 2 + y % 2)

    def tm_at(off, sign):
        return ((yh + off[0]) % 2) * 8 + ((z + sign * off[1] + 4) % 4) * 2 + (c + off[2]) % 2

    def along(axis, hop):
        there = list(at)
        there[axis] = (there[axis] + hop) % 4
        return device(*there, c)

    partner = device(x, y, z, 1 - c)

    local = [
        pltpu.make_async_copy(q, qc.at[0], lsem.at[0]),
        pltpu.make_async_copy(cot, qc.at[1], lsem.at[1]),
        pltpu.make_async_copy(wk, w.at[0], lsem.at[2]),
        pltpu.make_async_copy(wv, w.at[1], lsem.at[3]),
        pltpu.make_async_copy(
            enc.at[:, pl.ds(pl.multiple_of(16 * tm, 16), 8)], e.at[0, pl.ds(0, 5)], lsem.at[4]
        ),
        pltpu.make_async_copy(
            enc.at[:, pl.ds(pl.multiple_of(16 * tm + 8, 8), 8)], e.at[1, pl.ds(0, 5)], lsem.at[5]
        ),
    ]
    barrier = pltpu.get_barrier_semaphore()
    peers = [(tm_at(off, 1), dp) for off in OFFS[1:]]
    peers += [along(0, h) for h in (1, 2, 3)] + [along(1, h) for h in (1, 3)]
    for peer in peers:
        pl.semaphore_signal(barrier, inc=1, device_id=peer, device_id_type=MESH)
    for copy in local:
        copy.start()
    pl.semaphore_wait(barrier, len(peers))

    def exchange(h, k, target):
        return pltpu.make_async_remote_copy(
            src_ref=enc.at[:, pl.ds(pl.multiple_of(16 * target + 8 * h, 8), 8)],
            dst_ref=e.at[h, pl.ds(5 * k, 5)],
            send_sem=xs.at[h, k],
            recv_sem=xr.at[h, k],
            device_id=(target, dp),
            device_id_type=MESH,
        )

    sends = []
    for h in range(2):
        for k, off in enumerate(OFFS):
            if k:
                copy = exchange(h, k, tm_at(off, 1))
                copy.start()
                sends.append(copy)
    for copy in local[:2]:
        copy.wait()

    def to_partner(src, dst, k):
        return pltpu.make_async_remote_copy(
            src_ref=src, dst_ref=dst, send_sem=ds.at[k], recv_sem=dr.at[k],
            device_id=partner, device_id_type=MESH,
        )

    operands = []
    for h in range(2):
        half = pl.ds(256 * h, 256)
        copy = to_partner(qc.at[1 - c, half], r.at[h, pl.ds(256, 256)], h)
        copy.start()
        sends.append(copy)
        operands.append(copy)
        copy = pltpu.make_async_copy(qc.at[c, half], r.at[h, pl.ds(0, 256)], lsem.at[6 + h])
        copy.start()
        local.append(copy)

    column = lax.broadcasted_iota(jnp.int32, (1, 256), 1) // 32
    row = lax.broadcasted_iota(jnp.int32, (40, 256), 0)
    same = row % 8 == column
    for h in range(2):
        limit = jnp.zeros((1, 256), jnp.int32)
        for b in range(8):
            limit = jnp.where(column == b, lens[8 * h + b], limit)
        for k, off in enumerate(OFFS):
            position = 5 * tm_at(off, -1) + row // 8
            st[h, pl.ds(40 * k, 40), :] = jnp.where(same & (position < limit), 0.0, -1e30)

    for copy in local[2:]:
        copy.wait()

    def stream(h):
        def arrive(j, carry):
            top, total, dots = carry
            for i in range(3):
                k = 3 * j + 1 + i
                pltpu.make_async_remote_copy(
                    src_ref=enc.at[:, pl.ds(0, 8)],
                    dst_ref=e.at[h, pl.ds(5 * k, 5)],
                    send_sem=xs.at[h, k],
                    recv_sem=xr.at[h, k],
                    device_id=partner,
                    device_id_type=MESH,
                ).wait_recv()
            rows = pl.ds(pl.multiple_of(128 * j, 128), 128)
            block = e[h, pl.ds(16 * j, 16)].reshape(128, 1024)
            et[h, :, rows] = block.T
            keys = nn(block, w[0]).astype(BF16)
            values = nn(block, w[1]).astype(BF16)
            v[h, rows, :] = values
            scores = nt(keys, qc[0, pl.ds(256 * h, 256)]) * (1.0 / 32.0) + st[h, rows, :]
            st[h, rows, :] = scores
            slope = nt(values, qc[1, pl.ds(256 * h, 256)])
            gp[h, rows, :] = slope
            scores = scores.reshape(16, 8, 256)
            peak = jnp.maximum(top, jnp.max(scores, axis=0))
            weights = jnp.exp(scores - peak)
            shrink = jnp.exp(top - peak)
            total = total * shrink + jnp.sum(weights, axis=0)
            dots = dots * shrink + jnp.sum(weights * slope.reshape(16, 8, 256), axis=0)
            return peak, total, dots

        zero = jnp.zeros((8, 256), F32)
        top, total, dots = lax.fori_loop(0, 5, arrive, (jnp.full((8, 256), -1e30, F32), zero, zero))
        peak = jnp.max(top, axis=0, keepdims=True)
        shrink = jnp.exp(top - peak)
        scale = 1.0 / jnp.sum(total * shrink, axis=0, keepdims=True)
        mean = jnp.sum(dots * shrink, axis=0, keepdims=True) * scale

        def normalise(j, carry):
            rows = pl.ds(pl.multiple_of(128 * j, 128), 128)
            probs = jnp.exp(st[h, rows, :] - peak) * scale
            pg[h, 1, rows, :] = probs.astype(BF16)
            pg[h, 0, rows, :] = (probs * (gp[h, rows, :] - mean)).astype(BF16)
            return carry

        lax.fori_loop(0, 5, normalise, 0)

    def weigh(h, slot, rows):
        factor = jnp.where(slot == 0, 1.0 / 32.0, 1.0)
        return (nn(et[h, rows, :], pg[h, slot]) * factor).astype(BF16)

    def swap(h):
        swapped = []
        for i in range(2):
            rows = pl.ds(512 * i, 512)
            a_out[h, rows, :] = weigh(h, 1 - c, rows)
            copy = to_partner(a_out.at[h, rows], a.at[h, rows, pl.ds(256, 256)], 2 + 2 * h + i)
            copy.start()
            sends.append(copy)
            swapped.append(copy)
        a[h, :, 0:256] = weigh(h, c, pl.ds(0, 1024))
        swapped.append(operands[h])
        return swapped

    stream(0)
    for copy in swap(0):
        copy.wait_recv()
    def first_half(j, carry):
        rows = pl.ds(pl.multiple_of(256 * j, 256), 256)
        part[rows, :] = nn(a[0, rows, :], r[0])
        return carry

    lax.fori_loop(0, 4, first_half, 0)
    stream(1)
    last = swap(1)
    for copy in last:
        copy.wait_recv()

    def pick(axis, value):
        return value[axis] * (1 - c) + value[(axis + 1) % 3] * c

    def there(axis, hop):
        place = [
            (at[i] + hop * ((1 - c) if i == axis else c if i == (axis + 1) % 3 else 0)) % 4
            for i in range(3)
        ]
        return device(*place, c)

    copies = {}

    def hop_copy(f, phase, h, axis, src, dst):
        copy = pltpu.make_async_remote_copy(
            src_ref=src, dst_ref=dst, send_sem=gs.at[f, phase, h], recv_sem=gr.at[f, phase, h],
            device_id=there(axis, HOPS[h]), device_id_type=MESH,
        )
        copy.start()
        sends.append(copy)
        copies[f, phase, h] = copy

    def arrived(f, phase):
        for h in range(3):
            copies[f, phase, h].wait_recv()

    def turned(axis, hop, size, start=0):
        return pl.multiple_of(start + ((pick(axis, at) + hop) % 4) * size, size)

    forwards = []

    def own_terms(flows):
        first, last = FLOWS[flows[0]][0], FLOWS[flows[-1]][1]

        def second_half(j, carry):
            rows = pl.ds(pl.multiple_of(TALL * j, TALL), TALL)
            term = part[rows, first:last] + nn(a[1, rows, :], r[1, :, first:last])
            part[rows, first:last] = term
            snd[rows, first:last] = term.astype(BF16)
            return carry

        lax.fori_loop(0, 1024 // TALL, second_half, 0)
        for f in flows:
            for h in range(3):
                lo, hi, order, start, size = FLOWS[f]
                cols = pl.ds(lo, hi - lo)
                src = snd.at[pl.ds(turned(order[0], HOPS[h], size, start), size), cols]
                hop_copy(f, 0, h, order[0], src, rcv.at[h, pl.ds(start // 4, size), cols])

    def second_axis(flows):
        for f in flows:
            lo, hi, order, start, size = FLOWS[f]
            cols = pl.ds(lo, hi - lo)
            base, less = start // 4, size // 4
            arrived(f, 0)
            sums = part[pl.ds(turned(order[0], 0, size, start), size), lo:hi]
            for h in range(3):
                sums = sums + rcv[h, base : base + size, lo:hi].astype(F32)
            own[base : base + size, lo:hi] = sums
            snd2[base : base + size, lo:hi] = sums.astype(BF16)
            for h in range(3):
                src = snd2.at[pl.ds(turned(order[1], HOPS[h], less, base), less), cols]
                hop_copy(f, 1, h, order[1], src, rcv2.at[h, pl.ds(start // 16, less), cols])

    def third_axis(flows):
        for f in flows:
            lo, hi, order, start, size = FLOWS[f]
            base, less = start // 16, size // 4
            arrived(f, 1)
            sums = own[pl.ds(turned(order[1], 0, less, start // 4), less), lo:hi]
            for h in range(3):
                sums = sums + rcv2[h, base : base + less, lo:hi].astype(F32)
            mine = pick(order[2], at)
            last_sums[mine, base : base + less, lo:hi] = sums.astype(BF16)
            block = last_sums.at[mine, pl.ds(base, less), pl.ds(lo, hi - lo)]
            for h in range(3):
                hop_copy(f, 2, h, order[2], block, block)

    def back_second(flows):
        for f in flows:
            lo, hi, order, start, size = FLOWS[f]
            base, less = start // 16, size // 4
            arrived(f, 2)
            sums = last_sums[0, base : base + less, lo:hi].astype(F32)
            for i in range(1, 4):
                sums = sums + last_sums[i, base : base + less, lo:hi].astype(F32)
            first = start + pick(order[0], at) * size + pick(order[1], at) * less
            rows = pl.ds(pl.multiple_of(first, less), less)
            res[c, rows, lo:hi] = sums.astype(BF16)
            block = res.at[c, rows, pl.ds(lo, hi - lo)]
            for h in range(3):
                hop_copy(f, 3, h, order[1], block, block)

    def gathered(f, hop):
        lo, hi, order, start, size = FLOWS[f]
        return res.at[c, pl.ds(turned(order[0], hop, size, start), size), pl.ds(lo, hi - lo)]

    def forward(f, h):
        block = gathered(f, 4 - HOPS[h] if h < 3 else 0)
        copy = pltpu.make_async_remote_copy(
            src_ref=block, dst_ref=block, send_sem=fs.at[f, h], recv_sem=fr.at[f, h],
            device_id=partner, device_id_type=MESH,
        )
        copy.start()
        sends.append(copy)
        forwards.append(copy)

    def back_first(flows):
        for f in flows:
            arrived(f, 3)
            block = gathered(f, 0)
            for h in BACK:
                hop_copy(f, 4, h, FLOWS[f][2][0], block, block)
        for f in flows:
            forward(f, 3)

    def to_other_core(flows):
        for h in BACK:
            for f in flows:
                copies[f, 4, h].wait_recv()
                forward(f, h)

    def contexts(flows):
        for h in range(2):
            ctx[pl.ds(256 * h, 256), :] = tn(pg[h, 1], v[h]).astype(BF16)

    def drain(flows):
        done = marks[-4]
        for copy in sends[:done]:
            copy.wait_send()
        del sends[:done]
        marks[:] = [0] * 4

    marks = [0] * 4
    steps = (
        own_terms, second_axis, third_axis, back_second, back_first, to_other_core, contexts, drain,
    )
    for step, p in SCHEDULE:
        if step < 7:
            marks.append(len(sends))
        steps[step](PARTS[p])
    for copy in forwards:
        copy.wait_recv()
    for copy in sends:
        copy.wait_send()


def finish(sums, context, key_grad, value_grad, context_out, wide, sem):
    copies = [pltpu.make_async_copy(context, context_out, sem.at[8])]
    copies[0].start()
    for i, out in enumerate((key_grad, value_grad)):
        for j in range(4):
            rows = pl.ds(256 * j, 256)
            wide[i, rows, :] = sums[i, rows, :].astype(F32)
            copy = pltpu.make_async_copy(wide.at[i, rows], out.at[rows], sem.at[4 * i + j])
            copy.start()
            copies.append(copy)
    for copy in copies:
        copy.wait()


def body(encoded, queries, cotangent, lengths, key_weight, value_weight):
    any_space = pl.BlockSpec(memory_space=pltpu.HBM)
    dma = pltpu.SemaphoreType.DMA
    grads, context = pl.pallas_call(
        kernel,
        out_shape=(
            pltpu.VMEM((2, 1024, 1024), BF16),
            pltpu.VMEM((512, 1024), BF16),
        ),
        in_specs=[any_space] * 3 + [pl.BlockSpec(memory_space=pltpu.SMEM)] + [any_space] * 2,
        out_specs=(pl.BlockSpec(memory_space=pltpu.VMEM), pl.BlockSpec(memory_space=pltpu.VMEM)),
        scratch_shapes=[
            pltpu.VMEM((2, 80, 8, 1024), BF16),
            pltpu.VMEM((2, 1024, 640), BF16),
            pltpu.VMEM((2, 640, 1024), BF16),
            pltpu.VMEM((2, 640, 256), F32),
            pltpu.VMEM((2, 640, 256), F32),
            pltpu.VMEM((2, 2, 640, 256), BF16),
            pltpu.VMEM((2, 512, 1024), BF16),
            pltpu.VMEM((2, 1024, 1024), BF16),
            pltpu.VMEM((2, 1024, 512), BF16),
            pltpu.VMEM((2, 1024, 256), BF16),
            pltpu.VMEM((2, 512, 1024), BF16),
            pltpu.VMEM((1024, 1024), F32),
            pltpu.VMEM((256, 1024), F32),
            pltpu.VMEM((1024, 1024), BF16),
            pltpu.VMEM((256, 1024), BF16),
            pltpu.VMEM((3, 256, 1024), BF16),
            pltpu.VMEM((3, 64, 1024), BF16),
            pltpu.VMEM((4, 64, 1024), BF16),
            dma((8,)), dma((2, 16)), dma((2, 16)), dma((6,)), dma((6,)),
            dma((9, 5, 3)), dma((9, 5, 3)), dma((9, 4)), dma((9, 4)),
        ],
        compiler_params=pltpu.CompilerParams(
            collective_id=0, has_side_effects=True, vmem_limit_bytes=50 * 2**20
        ),
    )(
        jnp.transpose(encoded, (1, 0, 2)),
        queries.reshape(512, 1024),
        cotangent.reshape(512, 1024),
        lengths,
        key_weight,
        value_weight,
    )
    key_grad, value_grad, context = pl.pallas_call(
        finish,
        out_shape=(
            jax.ShapeDtypeStruct((1024, 1024), F32),
            jax.ShapeDtypeStruct((1024, 1024), F32),
            jax.ShapeDtypeStruct((512, 1024), BF16),
        ),
        in_specs=[pl.BlockSpec(memory_space=pltpu.VMEM)] * 2,
        out_specs=(any_space,) * 3,
        scratch_shapes=[pltpu.VMEM((2, 1024, 1024), F32), dma((9,))],
        compiler_params=pltpu.CompilerParams(vmem_limit_bytes=16 * 2**20),
    )(grads, context)
    return context.reshape(16, 32, 1024), key_grad, value_grad


def solution(mesh):
    return jax.shard_map(
        body,
        mesh=mesh,
        in_specs=(
            P("dp", "tm", None),
            P(("dp", "tm"), None, None),
            P(("dp", "tm"), None, None),
            P(("dp", "tm")),
            P(),
            P(),
        ),
        out_specs=(P(("dp", "tm"), None, None), P(), P()),
        check_vma=False,
    )
```

```python
import functools

import jax
import jax.numpy as jnp
from jax import lax
from jax.experimental import pallas as pl
from jax.experimental.pallas import tpu as pltpu
from jax.sharding import PartitionSpec as P

MESH = pl.DeviceIdType.MESH
F32, BF16 = jnp.float32, jnp.bfloat16
OFFS = (
    (0, 0, 0), (0, 0, 1),
    (0, 1, 0), (0, 3, 0), (1, 0, 0), (0, 1, 1), (0, 3, 1), (1, 0, 1),
    (1, 1, 0), (1, 3, 0), (0, 2, 0), (1, 1, 1), (1, 3, 1), (0, 2, 1),
    (1, 2, 0), (1, 2, 1),
)
FLOWS = (
    (0, 128, (0, 1, 2), 0, 256), (128, 256, (1, 2, 0), 0, 256),
    (256, 384, (2, 0, 1), 0, 256), (384, 512, (0, 1, 2), 0, 256),
    (512, 640, (1, 2, 0), 0, 256), (640, 768, (2, 0, 1), 0, 256),
    (768, 896, (0, 1, 2), 0, 256),
    (896, 1024, (1, 2, 0), 0, 128), (896, 1024, (2, 0, 1), 512, 128),
)
PARTS = ((0, 1), (2, 3), (4, 5), (6, 7, 8))
HOPS = (2, 1, 3)
BACK = (0, 1, 2)
TALL = 1024
SCHEDULE = ((0, 0), (0, 1), (0, 2), (0, 3), (6, 0), (7, 0)) + tuple((s, p) for s in range(1, 5) for p in range(4)) + (
    (7, 0), (5, 0), (5, 1), (5, 2), (5, 3),
)


def nt(a, b):
    return lax.dot_general(a, b, (((1,), (1,)), ((), ())), preferred_element_type=F32)


def nn(a, b):
    return jnp.dot(a, b, preferred_element_type=F32)


def tn(a, b):
    return lax.dot_general(a, b, (((0,), (0,)), ((), ())), preferred_element_type=F32)


def kernel(
    enc, q, cot, lens, wk, wv, res, ctx,
    es, e, et, v, st, gp, pg, qc, w, a, a_out, r, part, own, snd, snd2, rcv, rcv2, last_sums,
    lsem, xs, xr, ds, dr, gs, gr, fs, fr,
):
    tm, dp = lax.axis_index("tm"), lax.axis_index("dp")
    yh, z, c = tm // 8, (tm // 2) % 4, tm % 2
    x, y = dp // 2, yh * 2 + dp % 2
    at = (x, y, z)

    def device(x, y, z, c):
        return ((y // 2) * 8 + z * 2 + c, x * 2 + y % 2)

    def tm_at(off, sign):
        return ((yh + off[0]) % 2) * 8 + ((z + sign * off[1] + 4) % 4) * 2 + (c + off[2]) % 2

    def along(axis, hop):
        there = list(at)
        there[axis] = (there[axis] + hop) % 4
        return device(*there, c)

    partner = device(x, y, z, 1 - c)

    load = pltpu.make_async_copy(enc, es, lsem.at[4])
    load.start()
    local = [
        pltpu.make_async_copy(q, qc.at[0], lsem.at[0]),
        pltpu.make_async_copy(cot, qc.at[1], lsem.at[1]),
        pltpu.make_async_copy(wk, w.at[0], lsem.at[2]),
        pltpu.make_async_copy(wv, w.at[1], lsem.at[3]),
    ]
    barrier = pltpu.get_barrier_semaphore()
    peers = [(tm_at(off, 1), dp) for off in OFFS[1:]]
    peers += [along(0, h) for h in (1, 2, 3)] + [along(1, h) for h in (1, 3)]
    for peer in peers:
        pl.semaphore_signal(barrier, inc=1, device_id=peer, device_id_type=MESH)
    for copy in local:
        copy.start()
    load.wait()
    for h in range(2):
        rows = pl.ds(pl.multiple_of(16 * tm + 8 * h, 8), 8)
        copy = pltpu.make_async_copy(es.at[:, rows], e.at[h, pl.ds(0, 5)], lsem.at[5 + 3 * h])
        copy.start()
        local.append(copy)
    pl.semaphore_wait(barrier, len(peers))

    def exchange(h, k, target):
        return pltpu.make_async_remote_copy(
            src_ref=es.at[:, pl.ds(pl.multiple_of(16 * target + 8 * h, 8), 8)],
            dst_ref=e.at[h, pl.ds(5 * k, 5)],
            send_sem=xs.at[h, k],
            recv_sem=xr.at[h, k],
            device_id=(target, dp),
            device_id_type=MESH,
        )

    sends = []
    for h in range(2):
        for k, off in enumerate(OFFS):
            if k:
                copy = exchange(h, k, tm_at(off, 1))
                copy.start()
                sends.append(copy)
    for copy in local[:2]:
        copy.wait()

    def to_partner(src, dst, k):
        return pltpu.make_async_remote_copy(
            src_ref=src, dst_ref=dst, send_sem=ds.at[k], recv_sem=dr.at[k],
            device_id=partner, device_id_type=MESH,
        )

    operands = []
    for h in range(2):
        half = pl.ds(256 * h, 256)
        copy = to_partner(qc.at[1 - c, half], r.at[h, pl.ds(256, 256)], h)
        copy.start()
        sends.append(copy)
        operands.append(copy)
        copy = pltpu.make_async_copy(qc.at[c, half], r.at[h, pl.ds(0, 256)], lsem.at[6 + h])
        copy.start()
        local.append(copy)

    column = lax.broadcasted_iota(jnp.int32, (1, 256), 1) // 32
    row = lax.broadcasted_iota(jnp.int32, (40, 256), 0)
    same = row % 8 == column
    for h in range(2):
        limit = jnp.zeros((1, 256), jnp.int32)
        for b in range(8):
            limit = jnp.where(column == b, lens[8 * h + b], limit)
        for k, off in enumerate(OFFS):
            position = 5 * tm_at(off, -1) + row // 8
            st[h, pl.ds(40 * k, 40), :] = jnp.where(same & (position < limit), 0.0, -1e30)

    for copy in local[2:]:
        copy.wait()

    def stream(h):
        def arrive(j, carry):
            top, total, dots = carry
            for i in range(3):
                k = 3 * j + 1 + i
                pltpu.make_async_remote_copy(
                    src_ref=es.at[:, pl.ds(0, 8)],
                    dst_ref=e.at[h, pl.ds(5 * k, 5)],
                    send_sem=xs.at[h, k],
                    recv_sem=xr.at[h, k],
                    device_id=partner,
                    device_id_type=MESH,
                ).wait_recv()
            rows = pl.ds(pl.multiple_of(128 * j, 128), 128)
            block = e[h, pl.ds(16 * j, 16)].reshape(128, 1024)
            et[h, :, rows] = block.T
            keys = nn(block, w[0]).astype(BF16)
            values = nn(block, w[1]).astype(BF16)
            v[h, rows, :] = values
            scores = nt(keys, qc[0, pl.ds(256 * h, 256)]) * (1.0 / 32.0) + st[h, rows, :]
            st[h, rows, :] = scores
            slope = nt(values, qc[1, pl.ds(256 * h, 256)])
            gp[h, rows, :] = slope
            scores = scores.reshape(16, 8, 256)
            peak = jnp.maximum(top, jnp.max(scores, axis=0))
            weights = jnp.exp(scores - peak)
            shrink = jnp.exp(top - peak)
            total = total * shrink + jnp.sum(weights, axis=0)
            dots = dots * shrink + jnp.sum(weights * slope.reshape(16, 8, 256), axis=0)
            return peak, total, dots

        zero = jnp.zeros((8, 256), F32)
        top, total, dots = lax.fori_loop(0, 5, arrive, (jnp.full((8, 256), -1e30, F32), zero, zero))
        peak = jnp.max(top, axis=0, keepdims=True)
        shrink = jnp.exp(top - peak)
        scale = 1.0 / jnp.sum(total * shrink, axis=0, keepdims=True)
        mean = jnp.sum(dots * shrink, axis=0, keepdims=True) * scale

        def normalise(j, carry):
            rows = pl.ds(pl.multiple_of(128 * j, 128), 128)
            probs = jnp.exp(st[h, rows, :] - peak) * scale
            pg[h, 1, rows, :] = probs.astype(BF16)
            pg[h, 0, rows, :] = (probs * (gp[h, rows, :] - mean)).astype(BF16)
            return carry

        lax.fori_loop(0, 5, normalise, 0)

    def weigh(h, slot, rows):
        factor = jnp.where(slot == 0, 1.0 / 32.0, 1.0)
        return (nn(et[h, rows, :], pg[h, slot]) * factor).astype(BF16)

    def swap(h):
        swapped = []
        for i in range(2):
            rows = pl.ds(512 * i, 512)
            a_out[h, rows, :] = weigh(h, 1 - c, rows)
            copy = to_partner(a_out.at[h, rows], a.at[h, rows, pl.ds(256, 256)], 2 + 2 * h + i)
            copy.start()
            sends.append(copy)
            swapped.append(copy)
        a[h, :, 0:256] = weigh(h, c, pl.ds(0, 1024))
        swapped.append(operands[h])
        return swapped

    stream(0)
    for copy in swap(0):
        copy.wait_recv()
    def first_half(j, carry):
        rows = pl.ds(pl.multiple_of(256 * j, 256), 256)
        part[rows, :] = nn(a[0, rows, :], r[0])
        return carry

    lax.fori_loop(0, 4, first_half, 0)
    stream(1)
    last = swap(1)
    for copy in last:
        copy.wait_recv()

    def pick(axis, value):
        return value[axis] * (1 - c) + value[(axis + 1) % 3] * c

    def there(axis, hop):
        place = [
            (at[i] + hop * ((1 - c) if i == axis else c if i == (axis + 1) % 3 else 0)) % 4
            for i in range(3)
        ]
        return device(*place, c)

    copies = {}

    def hop_copy(f, phase, h, axis, src, dst):
        copy = pltpu.make_async_remote_copy(
            src_ref=src, dst_ref=dst, send_sem=gs.at[f, phase, h], recv_sem=gr.at[f, phase, h],
            device_id=there(axis, HOPS[h]), device_id_type=MESH,
        )
        copy.start()
        sends.append(copy)
        copies[f, phase, h] = copy

    def arrived(f, phase):
        for h in range(3):
            copies[f, phase, h].wait_recv()

    def turned(axis, hop, size, start=0):
        return pl.multiple_of(start + ((pick(axis, at) + hop) % 4) * size, size)

    forwards = []

    def own_terms(flows):
        first, last = FLOWS[flows[0]][0], FLOWS[flows[-1]][1]

        def second_half(j, carry):
            rows = pl.ds(pl.multiple_of(TALL * j, TALL), TALL)
            term = part[rows, first:last] + nn(a[1, rows, :], r[1, :, first:last])
            part[rows, first:last] = term
            snd[rows, first:last] = term.astype(BF16)
            return carry

        lax.fori_loop(0, 1024 // TALL, second_half, 0)
        for f in flows:
            for h in range(3):
                lo, hi, order, start, size = FLOWS[f]
                cols = pl.ds(lo, hi - lo)
                src = snd.at[pl.ds(turned(order[0], HOPS[h], size, start), size), cols]
                hop_copy(f, 0, h, order[0], src, rcv.at[h, pl.ds(start // 4, size), cols])

    def second_axis(flows):
        for f in flows:
            lo, hi, order, start, size = FLOWS[f]
            cols = pl.ds(lo, hi - lo)
            base, less = start // 4, size // 4
            arrived(f, 0)
            sums = part[pl.ds(turned(order[0], 0, size, start), size), lo:hi]
            for h in range(3):
                sums = sums + rcv[h, base : base + size, lo:hi].astype(F32)
            own[base : base + size, lo:hi] = sums
            snd2[base : base + size, lo:hi] = sums.astype(BF16)
            for h in range(3):
                src = snd2.at[pl.ds(turned(order[1], HOPS[h], less, base), less), cols]
                hop_copy(f, 1, h, order[1], src, rcv2.at[h, pl.ds(start // 16, less), cols])

    def third_axis(flows):
        for f in flows:
            lo, hi, order, start, size = FLOWS[f]
            base, less = start // 16, size // 4
            arrived(f, 1)
            sums = own[pl.ds(turned(order[1], 0, less, start // 4), less), lo:hi]
            for h in range(3):
                sums = sums + rcv2[h, base : base + less, lo:hi].astype(F32)
            mine = pick(order[2], at)
            last_sums[mine, base : base + less, lo:hi] = sums.astype(BF16)
            block = last_sums.at[mine, pl.ds(base, less), pl.ds(lo, hi - lo)]
            for h in range(3):
                hop_copy(f, 2, h, order[2], block, block)

    def back_second(flows):
        for f in flows:
            lo, hi, order, start, size = FLOWS[f]
            base, less = start // 16, size // 4
            arrived(f, 2)
            sums = last_sums[0, base : base + less, lo:hi].astype(F32)
            for i in range(1, 4):
                sums = sums + last_sums[i, base : base + less, lo:hi].astype(F32)
            first = start + pick(order[0], at) * size + pick(order[1], at) * less
            rows = pl.ds(pl.multiple_of(first, less), less)
            res[c, rows, lo:hi] = sums.astype(BF16)
            block = res.at[c, rows, pl.ds(lo, hi - lo)]
            for h in range(3):
                hop_copy(f, 3, h, order[1], block, block)

    def gathered(f, hop):
        lo, hi, order, start, size = FLOWS[f]
        return res.at[c, pl.ds(turned(order[0], hop, size, start), size), pl.ds(lo, hi - lo)]

    def forward(f, h):
        block = gathered(f, 4 - HOPS[h] if h < 3 else 0)
        copy = pltpu.make_async_remote_copy(
            src_ref=block, dst_ref=block, send_sem=fs.at[f, h], recv_sem=fr.at[f, h],
            device_id=partner, device_id_type=MESH,
        )
        copy.start()
        sends.append(copy)
        forwards.append(copy)

    def back_first(flows):
        for f in flows:
            arrived(f, 3)
            block = gathered(f, 0)
            for h in BACK:
                hop_copy(f, 4, h, FLOWS[f][2][0], block, block)
        for f in flows:
            forward(f, 3)

    def to_other_core(flows):
        for h in BACK:
            for f in flows:
                copies[f, 4, h].wait_recv()
                forward(f, h)

    def contexts(flows):
        for h in range(2):
            ctx[pl.ds(256 * h, 256), :] = tn(pg[h, 1], v[h]).astype(BF16)

    def drain(flows):
        done = marks[-4]
        for copy in sends[:done]:
            copy.wait_send()
        del sends[:done]
        marks[:] = [0] * 4

    marks = [0] * 4
    steps = (
        own_terms, second_axis, third_axis, back_second, back_first, to_other_core, contexts, drain,
    )
    for step, p in SCHEDULE:
        if step < 7:
            marks.append(len(sends))
        steps[step](PARTS[p])
    for copy in forwards:
        copy.wait_recv()
    for copy in sends:
        copy.wait_send()


def finish(sums, context, key_grad, value_grad, context_out, wide, sem):
    copies = [pltpu.make_async_copy(context, context_out, sem.at[8])]
    copies[0].start()
    for i, out in enumerate((key_grad, value_grad)):
        for j in range(4):
            rows = pl.ds(256 * j, 256)
            wide[i, rows, :] = sums[i, rows, :].astype(F32)
            copy = pltpu.make_async_copy(wide.at[i, rows], out.at[rows], sem.at[4 * i + j])
            copy.start()
            copies.append(copy)
    for copy in copies:
        copy.wait()


def body(encoded, queries, cotangent, lengths, key_weight, value_weight):
    any_space = pl.BlockSpec(memory_space=pltpu.HBM)
    dma = pltpu.SemaphoreType.DMA
    grads, context = pl.pallas_call(
        kernel,
        out_shape=(
            pltpu.VMEM((2, 1024, 1024), BF16),
            pltpu.VMEM((512, 1024), BF16),
        ),
        in_specs=[any_space] * 3 + [pl.BlockSpec(memory_space=pltpu.SMEM)] + [any_space] * 2,
        out_specs=(pl.BlockSpec(memory_space=pltpu.VMEM), pl.BlockSpec(memory_space=pltpu.VMEM)),
        scratch_shapes=[
            pltpu.VMEM((5, 256, 1024), BF16),
            pltpu.VMEM((2, 80, 8, 1024), BF16),
            pltpu.VMEM((2, 1024, 640), BF16),
            pltpu.VMEM((2, 640, 1024), BF16),
            pltpu.VMEM((2, 640, 256), F32),
            pltpu.VMEM((2, 640, 256), F32),
            pltpu.VMEM((2, 2, 640, 256), BF16),
            pltpu.VMEM((2, 512, 1024), BF16),
            pltpu.VMEM((2, 1024, 1024), BF16),
            pltpu.VMEM((2, 1024, 512), BF16),
            pltpu.VMEM((2, 1024, 256), BF16),
            pltpu.VMEM((2, 512, 1024), BF16),
            pltpu.VMEM((1024, 1024), F32),
            pltpu.VMEM((256, 1024), F32),
            pltpu.VMEM((1024, 1024), BF16),
            pltpu.VMEM((256, 1024), BF16),
            pltpu.VMEM((3, 256, 1024), BF16),
            pltpu.VMEM((3, 64, 1024), BF16),
            pltpu.VMEM((4, 64, 1024), BF16),
            dma((9,)), dma((2, 16)), dma((2, 16)), dma((6,)), dma((6,)),
            dma((9, 5, 3)), dma((9, 5, 3)), dma((9, 4)), dma((9, 4)),
        ],
        compiler_params=pltpu.CompilerParams(
            collective_id=0, has_side_effects=True, vmem_limit_bytes=50 * 2**20
        ),
    )(
        jnp.transpose(encoded, (1, 0, 2)),
        queries.reshape(512, 1024),
        cotangent.reshape(512, 1024),
        lengths,
        key_weight,
        value_weight,
    )
    key_grad, value_grad, context = pl.pallas_call(
        finish,
        out_shape=(
            jax.ShapeDtypeStruct((1024, 1024), F32),
            jax.ShapeDtypeStruct((1024, 1024), F32),
            jax.ShapeDtypeStruct((512, 1024), BF16),
        ),
        in_specs=[pl.BlockSpec(memory_space=pltpu.VMEM)] * 2,
        out_specs=(any_space,) * 3,
        scratch_shapes=[pltpu.VMEM((2, 1024, 1024), F32), dma((9,))],
        compiler_params=pltpu.CompilerParams(vmem_limit_bytes=16 * 2**20),
    )(grads, context)
    return context.reshape(16, 32, 1024), key_grad, value_grad


def solution(mesh):
    return jax.shard_map(
        body,
        mesh=mesh,
        in_specs=(
            P("dp", "tm", None),
            P(("dp", "tm"), None, None),
            P(("dp", "tm"), None, None),
            P(("dp", "tm")),
            P(),
            P(),
        ),
        out_specs=(P(("dp", "tm"), None, None), P(), P()),
        check_vma=False,
    )
```
